128 devices in a mesh: fsdp: 16 (over x, y), seq: 8 (over z, core).
Axes of the slice: x: 4, y: 4, z: 4, core: 2. Of those that a mesh axis runs over, the one named last changes fastest.
Arguments:
- tokens: bfloat16 [16, 4096, 4096], P('fsdp', 'seq'), may hold values from -72 to 72
- norm_gain: float32 [4096], replicated, may hold values from 0.1 to 1.9
- lru_proj: bfloat16 [4096, 2048], P(('fsdp', 'seq')), may hold values from -0.09375 to 0.09375
- gelu_proj: bfloat16 [4096, 2048], P(('fsdp', 'seq')), may hold values from -0.09375 to 0.09375
- conv_weight: float32 [4, 2048], replicated, may hold values from -3 to 3
- conv_bias: float32 [2048], replicated, may hold values from -3 to 3
- gate_weights: bfloat16 [2048, 512], P('seq'), may hold values from -0.375 to 0.375
- gate_bias: float32 [2, 2048], replicated, may hold values from -4 to 4
- decay_param: float32 [2048], replicated, may hold values from -13 to -2
Outputs:
- recurrent_out: bfloat16 [16, 4096, 2048], P('fsdp', 'seq')
The draws below stay inside these ranges and needn't reach their ends.
All inputs are finite; a program needn't handle non-finite values.
Results may differ from the reference program's by a relative error of at most 0.0051.
Values may be sent and summed in bfloat16 or wider, within the bound.
A program may use at most 128 MiB of HBM per device.

```python
import math
import jax
import jax.numpy as jnp
from jax import lax

D = 4096
BW = 256
H = 8
CONV = 4
TOK_DEV = 512
C = 2048
LENGTH = 4096
SEQS = 16


def draw_tokens(key, part):
    keys = jax.random.split(key, 3)
    shape = (SEQS, LENGTH, D)
    column_scale = jnp.exp(jax.random.uniform(keys[0], (D,), jnp.float32, math.log(0.3), math.log(3.0)))
    row_scale = jnp.exp(jax.random.uniform(keys[1], (SEQS, LENGTH, 1), jnp.float32, math.log(0.3), math.log(3.0)))
    base = jnp.clip(jax.random.normal(keys[2], shape, jnp.float32), -3.0, 3.0)
    return (base * row_scale * column_scale).astype(jnp.bfloat16)


def draw_decay_param(key, part):
    keys = jax.random.split(key, 3)
    shortest = min(40, TOK_DEV)
    slow_rate = jnp.exp(jax.random.uniform(keys[0], (C,), jnp.float32, math.log(0.05 / LENGTH), math.log(0.5 / LENGTH)))
    fast_rate = jnp.exp(jax.random.uniform(keys[1], (C,), jnp.float32, math.log(0.2 / shortest), math.log(0.5 / shortest)))
    share = 0.5
    picked = jax.random.uniform(keys[2], (C,), jnp.float32) < share
    rate = jnp.where(picked, fast_rate, slow_rate)
    return jnp.log(jnp.expm1(rate)).astype(jnp.float32)


def block_levels(key, dims, cuts, smallest, high):
    def one(position, blocks):
        draws = jax.random.uniform(jax.random.fold_in(jax.random.fold_in(key, 6), position), (blocks,), jnp.float32, smallest / len(cuts), high / len(cuts))
        return jnp.repeat(jnp.exp(draws), dims[position] // blocks).reshape((-1,) + (1,) * (len(dims) - position - 1))

    factor_of = one(*cuts[0])
    for cut in cuts[1:]:
        factor_of = factor_of * one(*cut)
    return factor_of


def noise(stream_key, extent, width, bound, cuts=(), kind=jnp.bfloat16):
    values = jax.random.normal(stream_key, extent, jnp.float32) * width
    if len(cuts) > 0:
        values = block_levels(stream_key, extent, cuts, -0.22, 0.18) * values
    return jnp.clip(values, min=-bound, max=bound).astype(kind)


def setup_inputs(seed: int = 0) -> dict:
    streams_of = jax.random.split(jax.random.key(seed), 10)
    return {
        "tokens": draw_tokens(jax.random.fold_in(streams_of[9], 71), 0),
        "norm_gain": jnp.clip(1.0 + 0.18 * jax.random.normal(streams_of[1], (D,), jnp.float32), 0.1, 1.9),
        "lru_proj": noise(streams_of[2], (D, C), D ** -0.5, 0.09375, ((0, 128),)),
        "gelu_proj": noise(streams_of[3], (D, C), D ** -0.5, 0.09375, ((0, 128),)),
        "conv_weight": noise(streams_of[4], (CONV, C), 0.5, 3.0, (), jnp.float32),
        "conv_bias": noise(streams_of[5], (C,), 0.5, 3.0, (), jnp.float32),
        "gate_weights": noise(streams_of[6], (C, 2 * BW), BW ** -0.5, 0.375, ((0, 8),)),
        "gate_bias": noise(streams_of[7], (2, C), 1.0, 4.0, (), jnp.float32),
        "decay_param": draw_decay_param(jax.random.fold_in(streams_of[9], 71), 0),
    }


def reference(tokens, norm_gain, lru_proj, gelu_proj, conv_weight, conv_bias, gate_weights, gate_bias, decay_param):

    def one_sequence(rows):
        values = rows.astype(jnp.float32)
        mean_square = lax.optimization_barrier(jnp.mean(values * values, axis=-1, keepdims=True))
        normed = (values * lax.rsqrt(mean_square + 1e-06) * norm_gain).astype(jnp.bfloat16)
        recurrent_in = jnp.dot(normed, lru_proj, preferred_element_type=jnp.float32).astype(jnp.bfloat16)
        gelu_in = jnp.dot(normed, gelu_proj, preferred_element_type=jnp.float32)
        padded = jnp.concatenate([jnp.zeros((CONV - 1, C), jnp.bfloat16), recurrent_in], axis=0)
        conv_sum = jnp.zeros((LENGTH, C), jnp.float32) + conv_bias
        for tap_index in range(CONV):
            begin = CONV - 1 - tap_index
            conv_sum = conv_sum + conv_weight[tap_index] * padded[begin:begin + LENGTH].astype(jnp.float32)
        conv_out = conv_sum.astype(jnp.bfloat16)
        gate_all = jnp.einsum('lhi,hij->lhj', conv_out.astype(jnp.float32).reshape(LENGTH, H, BW), gate_weights.astype(jnp.float32).reshape(H, BW, 2 * BW))
        input_gate = jax.nn.sigmoid(gate_all[:, :, :BW].reshape(LENGTH, C) + gate_bias[0])
        recur_gate = jax.nn.sigmoid(gate_all[:, :, BW:].reshape(LENGTH, C) + gate_bias[1])
        log_decay = -8.0 * jax.nn.softplus(decay_param) * recur_gate
        decay = jnp.exp(log_decay)
        driven = jnp.sqrt(-jnp.expm1(2.0 * log_decay)) * input_gate * conv_out.astype(jnp.float32)

        def advance(state, inputs):
            decay_now, driven_now = inputs
            state = decay_now * state + driven_now
            return (state, state)
        unused, states = lax.scan(advance, jnp.zeros((C,), jnp.float32), (decay, driven))
        return (states * jax.nn.gelu(gelu_in, approximate=True)).astype(jnp.bfloat16)
    return lax.map(one_sequence, tokens)
```

```python
import jax
import jax.numpy as jnp
from jax import lax
from jax.experimental import pallas as pl
from jax.experimental.pallas import tpu as pltpu
from jax.sharding import PartitionSpec as P

MESH = pl.DeviceIdType.MESH
HALO = 16
ROWS = 1024
WIDTH = 4096
HEADS = 4
BW = 256
CHUNKS = 8
X, Y, Z = 0, 1, 2
ORDERS = ((X, Y, Z), (Y, Z, X), (Z, X, Y))
PIECES = (
    (slice(0, 16), slice(0, 256)),
    (slice(16, 64), slice(0, 128)),
    (slice(16, 64), slice(128, 256)),
)
L_ROWS = 208
T_ROWS = 128
G_ROWS = 256


def piece(w, chunks, colour, phase, coords, half=None):
    order = ORDERS[colour]
    at = [chunks, None, None, None]
    for place, dim in enumerate(order):
        if place < phase:
            at[1 + dim] = pl.ds(0, 4)
            if place == 0 and half is not None:
                at[1 + dim] = pl.ds(2 * half, 2)
        else:
            at[1 + dim] = coords[dim]
    rows, cols = PIECES[colour]
    at.append(pl.ds(rows.start, rows.stop - rows.start))
    at.append(pl.ds(cols.start, cols.stop - cols.start))
    return w.at[tuple(at)]


def moved(coords, dim, by):
    new = list(coords)
    new[dim] = lax.rem(coords[dim] + (by + 4), 4)
    return new


class Ring:
    def __init__(self, w, chunks, colour, phase, coords, core, send, recv):
        self.w, self.chunks, self.colour, self.phase = w, chunks, colour, phase
        self.coords, self.core, self.send, self.recv = coords, core, send, recv
        self.dim = ORDERS[colour][phase]

    def device(self, by):
        x, y, z = moved(self.coords, self.dim, by)
        return (x * 4 + y, z * 2 + self.core)

    def block(self, by, half=None):
        chunks = self.chunks
        if self.phase == 0 and half is not None:
            chunks = pl.ds(4 * half, 4)
            half = None
        return piece(self.w, chunks, self.colour, self.phase, moved(self.coords, self.dim, by), half)

    def copy(self, hop, side, outgoing):
        way = 1 - 2 * side
        half = None if hop == 0 else side
        if outgoing:
            ref = self.block(-way * hop, half)
        else:
            ref = self.block(-way * (hop + 1), half)
        return pltpu.make_async_remote_copy(
            src_ref=ref,
            dst_ref=ref,
            send_sem=self.send.at[hop, side],
            recv_sem=self.recv.at[hop, side],
            device_id=self.device(way),
            device_id_type=MESH,
        )

    def start(self, hop):
        for side in range(2):
            self.copy(hop, side, True).start()

    def wait(self, hop):
        for side in range(2):
            self.copy(hop, side, False).wait_recv()

    def drain(self, hop):
        for side in range(2):
            self.copy(hop, side, True).wait_send()


def softplus_of(value):
    return jnp.maximum(value, 0.0) + jnp.log1p(jnp.exp(-jnp.abs(value)))


def one_minus_square(decay, twice):
    series = 1.0 + twice * (1.0 / 7.0)
    for divisor in (6.0, 5.0, 4.0, 3.0, 2.0):
        series = 1.0 + twice * (1.0 / divisor) * series
    return jnp.where(twice > -0.3, -twice * series, 1.0 - decay * decay)


def tile_scan(decay, driven):
    rows, cols = decay.shape
    place = lax.broadcasted_iota(jnp.int32, (rows, cols), 0)
    for step in (1, 2, 4):
        inside = (place % 8) >= step
        a_prev = jnp.where(inside, pltpu.roll(decay, step, 0), 1.0)
        b_prev = jnp.where(inside, pltpu.roll(driven, step, 0), 0.0)
        driven = decay * b_prev + driven
        decay = decay * a_prev
    group = decay.reshape(rows // 8, 8, cols)
    state = driven.reshape(rows // 8, 8, cols)
    last_a = jnp.broadcast_to(group[:, 7:8, :], group.shape)
    last_b = jnp.broadcast_to(state[:, 7:8, :], state.shape)
    run_a, run_b = last_a, last_b
    step = 1
    while step < rows // 8:
        ones = jnp.ones((step, 8, cols), jnp.float32)
        zeros = jnp.zeros((step, 8, cols), jnp.float32)
        a_prev = jnp.concatenate([ones, run_a[:-step]], axis=0)
        b_prev = jnp.concatenate([zeros, run_b[:-step]], axis=0)
        run_b = run_a * b_prev + run_b
        run_a = run_a * a_prev
        step *= 2
    ones = jnp.ones((1, 8, cols), jnp.float32)
    zeros = jnp.zeros((1, 8, cols), jnp.float32)
    before_a = jnp.concatenate([ones, run_a[:-1]], axis=0)
    before_b = jnp.concatenate([zeros, run_b[:-1]], axis=0)
    state = (state + group * before_b).reshape(rows, cols)
    group = (group * before_a).reshape(rows, cols)
    return group, state, run_a[-1], run_b[-1]


def body(
    tokens, gain, lru, gelu, conv_w, conv_b, gates, gate_b, decay_p, out,
    xn, w, gate_v, rec, local, cumul, outs, ends,
    own_sem, p1_send, p1_recv, p2_send, p2_recv, p3_send, p3_recv,
    tok_sem, halo_sem, gate_send, gate_recv, end_send, end_recv, out_sem, out_recv,
):
    fsdp = lax.axis_index("fsdp")
    seq = lax.axis_index("seq")
    x, y = fsdp // 4, fsdp % 4
    z, core = seq // 2, seq % 2
    other = 1 - core
    coords = [x, y, z]
    partner = (fsdp, z * 2 + other)

    barrier = pltpu.get_barrier_semaphore()
    for dim in (X, Y):
        for by in (1, -1):
            nx, ny, nz = moved(coords, dim, by)
            pl.semaphore_signal(
                barrier, inc=1, device_id=(nx * 4 + ny, nz * 2 + core), device_id_type=MESH
            )
    for by in range(1, 8):
        pl.semaphore_signal(
            barrier, inc=1, device_id=(fsdp, lax.rem(seq + by, 8)), device_id_type=MESH
        )

    def own_copies(mine):
        found = []
        for mat, source in enumerate((lru, gelu)):
            for head in range(HEADS):
                side = core if mine else other
                first = pl.multiple_of(side * (HEADS * BW) + head * BW, BW)
                found.append(
                    (
                        source.at[:, pl.ds(first, BW)],
                        w.at[2 * head + mat, x, y, z, pl.ds(pl.multiple_of(core * 32, 32), 32), :],
                        2 * head + mat,
                    )
                )
        return found

    local_copies = [
        pltpu.make_async_copy(src, dst, own_sem.at[0, n]) for src, dst, n in own_copies(True)
    ]
    for copy in local_copies:
        copy.start()
    my_rows = pl.ds(pl.multiple_of(HALO + core * 512, 16), 512)
    my_tokens = pltpu.make_async_copy(tokens.at[0], xn.at[my_rows, :], tok_sem.at[0])
    my_tokens.start()

    pl.semaphore_wait(barrier, 11)

    far_copies = [
        pltpu.make_async_remote_copy(
            src_ref=src,
            dst_ref=dst,
            send_sem=own_sem.at[1, n],
            recv_sem=own_sem.at[2, n],
            device_id=partner,
            device_id_type=MESH,
        )
        for src, dst, n in own_copies(False)
    ]
    for copy in far_copies:
        copy.start()
    for n, copy in enumerate(local_copies):
        copy.wait()
    other_rows = pl.ds(pl.multiple_of(other * 32, 32), 32)
    for n in range(CHUNKS):
        landed = w.at[n, x, y, z, other_rows, :]
        pltpu.make_async_copy(landed, landed, own_sem.at[2, n]).wait()

    def ring(phase, n, colour):
        send, recv = ((p1_send, p1_recv), (p2_send, p2_recv), (p3_send, p3_recv))[phase]
        if phase == 0:
            return Ring(w, pl.ds(0, CHUNKS), colour, 0, coords, core, send.at[colour], recv.at[colour])
        return Ring(w, n, colour, phase, coords, core, send.at[colour], recv.at[n, colour])

    def start(phase, n, hop):
        for colour in range(3):
            ring(phase, n, colour).start(hop)

    def wait(phase, n, hop):
        for colour in range(3):
            ring(phase, n, colour).wait(hop)

    start(0, None, 0)

    give_tokens = pltpu.make_async_remote_copy(
        src_ref=tokens.at[0],
        dst_ref=xn.at[my_rows, :],
        send_sem=tok_sem.at[1],
        recv_sem=tok_sem.at[2],
        device_id=partner,
        device_id_type=MESH,
    )
    give_tokens.start()

    def halo_copy(to_core):
        return pltpu.make_async_remote_copy(
            src_ref=tokens.at[0, pl.ds(512 - HALO, HALO), :],
            dst_ref=xn.at[pl.ds(0, HALO), :],
            send_sem=halo_sem.at[to_core],
            recv_sem=halo_sem.at[2],
            device_id=(fsdp, lax.rem(z + 1, 4) * 2 + to_core),
            device_id_type=MESH,
        )

    @pl.when(core == 1)
    def _():
        halo_copy(0).start()
        halo_copy(1).start()

    wait(0, None, 0)
    start(0, None, 1)

    kind = z // 2
    slot = (z % 2) * 2 + core

    def gate_copy(by):
        return pltpu.make_async_remote_copy(
            src_ref=gates,
            dst_ref=gate_v.at[slot],
            send_sem=gate_send.at[by],
            recv_sem=gate_recv.at[slot],
            device_id=(fsdp, lax.rem(z + by, 4) * 2 + kind),
            device_id_type=MESH,
        )

    def gate_local():
        return pltpu.make_async_copy(gates, gate_v.at[slot], gate_recv.at[slot])

    @pl.when(core == kind)
    def _():
        gate_local().start()

    @pl.when(core != kind)
    def _():
        gate_copy(0).start()

    wait(0, None, 1)
    start(1, 0, 0)
    start(1, 1, 0)
    start(1, 2, 0)
    for by in range(1, 4):
        gate_copy(by).start()

    my_tokens.wait()
    give_tokens.wait_recv()
    halo_copy(0).wait_recv()

    wait(1, 0, 0)
    start(1, 0, 1)
    wait(1, 1, 0)
    start(1, 1, 1)

    def norm_tile(i, _):
        rows = pl.ds(pl.multiple_of(i * 16, 16), 16)
        value = xn[rows, :].astype(jnp.float32)
        mean = jnp.mean(value * value, axis=-1, keepdims=True)
        normed = value * lax.rsqrt(mean + 1e-06) * gain[...]
        keep = jnp.where(jnp.logical_and(i == 0, z == 0), 0.0, 1.0)
        xn[rows, :] = (normed * keep).astype(jnp.bfloat16)
        return 0

    def norm(first, last):
        lax.fori_loop(first, last, norm_tile, 0)

    norm(0, 20)
    wait(1, 0, 1)
    start(2, 0, 0)
    wait(1, 2, 0)
    start(1, 2, 1)
    start(1, 3, 0)
    norm(20, 65)

    def columns(head):
        return pl.ds(pl.multiple_of(core * (HEADS * BW) + head * BW, BW), BW)

    def lru_chunk(head):
        n = 2 * head

        def rows_of(i, _):
            rows = pl.ds(pl.multiple_of(i * L_ROWS, 16), L_ROWS)
            value = jnp.dot(
                xn[rows, :], w[n].reshape(WIDTH, BW), preferred_element_type=jnp.float32
            )
            rec[rows, :] = value.astype(jnp.bfloat16).astype(jnp.float32)
            return 0

        lax.fori_loop(0, (HALO + ROWS) // L_ROWS, rows_of, 0)
        cols = columns(head)
        taps = conv_w[:, cols]
        bias = conv_b[:, cols]
        g_bias = gate_b[:, cols]
        rate = -8.0 * softplus_of(decay_p[:, cols])
        gate_block = gates_of(head)

        def tile(i, carry):
            carry_a, carry_b = carry
            first = pl.multiple_of(i * T_ROWS + (HALO - 8), 8)
            value = rec[pl.ds(first, T_ROWS + 8), :]
            total = jnp.zeros((T_ROWS, BW), jnp.float32) + bias
            for tap in range(4):
                total = total + taps[tap : tap + 1, :] * value[8 - tap : 8 - tap + T_ROWS, :]
            conv = total.astype(jnp.bfloat16)
            gate = jnp.dot(conv, gate_block, preferred_element_type=jnp.float32)
            input_gate = jax.nn.sigmoid(gate[:, :BW] + g_bias[0:1, :])
            recur_gate = jax.nn.sigmoid(gate[:, BW:] + g_bias[1:2, :])
            log_decay = rate * recur_gate
            decay = jnp.exp(log_decay)
            driven = (
                jnp.sqrt(one_minus_square(decay, 2.0 * log_decay))
                * input_gate
                * conv.astype(jnp.float32)
            )
            within_a, within_b, tile_a, tile_b = tile_scan(decay, driven)
            rows = pl.ds(pl.multiple_of(i * T_ROWS, T_ROWS), T_ROWS)
            local[head % 2, rows, :] = within_b + within_a * carry_b[0:1, :]
            cumul[head % 2, rows, :] = within_a * carry_a[0:1, :]
            return tile_a * carry_a, tile_b + tile_a * carry_b

        begin = (jnp.ones((8, BW), jnp.float32), jnp.zeros((8, BW), jnp.float32))
        end_a, end_b = lax.fori_loop(0, ROWS // T_ROWS, tile, begin)
        ends[head, z, 0, :, :] = end_a
        ends[head, z, 1, :, :] = end_b

    def gates_of(head):
        return gate_v[head]

    def end_copy(head, by):
        return pltpu.make_async_remote_copy(
            src_ref=ends.at[head, z],
            dst_ref=ends.at[head, z],
            send_sem=end_send.at[head, by - 1],
            recv_sem=end_recv.at[head, by - 1],
            device_id=(fsdp, lax.rem(z + by, 4) * 2 + core),
            device_id_type=MESH,
        )

    def end_landed(head, by):
        source = lax.rem(z + 4 - by, 4)
        landed = ends.at[head, source]
        pltpu.make_async_copy(landed, landed, end_recv.at[head, by - 1]).wait()

    def out_copy(head, i, far):
        side = other if far else core
        src = outs.at[head, pl.ds(pl.multiple_of(side * 512 + i * G_ROWS, G_ROWS), G_ROWS), :]
        dst = out.at[0, pl.ds(i * G_ROWS, G_ROWS), columns(head)]
        if far:
            return pltpu.make_async_remote_copy(
                src_ref=src,
                dst_ref=dst,
                send_sem=out_sem.at[1, head, i],
                recv_sem=out_recv.at[head, i],
                device_id=partner,
                device_id_type=MESH,
            )
        return pltpu.make_async_copy(src, dst, out_sem.at[0, head, i])

    def gelu_chunk(head):
        n = 2 * head + 1
        for by in range(1, 4):
            end_landed(head, by)
        begin = jnp.zeros((8, BW), jnp.float32)
        for source in range(3):
            after = ends[head, source, 0] * begin + ends[head, source, 1]
            begin = jnp.where(source < z, after, begin)
        weight = w[n].reshape(WIDTH, BW)
        for far in (True, False):
            side = other if far else core
            for i in range(2):
                first = pl.multiple_of(side * 512 + i * G_ROWS, G_ROWS)
                rows = pl.ds(first, G_ROWS)
                gelu_in = jnp.dot(
                    xn[pl.ds(pl.multiple_of(first + HALO, 16), G_ROWS), :],
                    weight,
                    preferred_element_type=jnp.float32,
                )
                state = local[head % 2, rows, :] + cumul[head % 2, rows, :] * begin[0:1, :]
                inner = gelu_in * (
                    0.7978845608028654 + (0.7978845608028654 * 0.044715) * (gelu_in * gelu_in)
                )
                part = 0.5 * gelu_in * (1.0 + jnp.tanh(inner))
                outs[head, rows, :] = (state * part).astype(jnp.bfloat16)
                out_copy(head, i, far).start()

    for j in range(4):
        landed = gate_v.at[j]
        if j == 0:
            pass

    def compute(n):
        head = n // 2
        if n == 0:
            for j in range(HEADS):
                pltpu.make_async_copy(gate_v.at[j], gate_v.at[j], gate_recv.at[j]).wait()
        if n % 2 == 0:
            lru_chunk(head)
            for by in range(1, 4):
                end_copy(head, by).start()
        else:
            gelu_chunk(head)

    for k in range(CHUNKS + 1):
        if k + 1 < CHUNKS:
            wait(1, k + 1, 1)
            start(2, k + 1, 0)
        if k < CHUNKS:
            wait(2, k, 0)
            start(2, k, 1)
        if k + 4 < CHUNKS:
            start(1, k + 4, 0)
        if k + 3 < CHUNKS:
            wait(1, k + 3, 0)
            start(1, k + 3, 1)
        if k >= 1:
            wait(2, k - 1, 1)
            compute(k - 1)

    for head in range(HEADS):
        for i in range(2):
            out_copy(head, i, False).wait()
            out_copy(head, i, True).wait_send()
            landed = out.at[0, pl.ds(i * G_ROWS, G_ROWS), pl.ds(pl.multiple_of(other * (HEADS * BW) + head * BW, BW), BW)]
            pltpu.make_async_copy(landed, landed, out_recv.at[head, i]).wait()
        for by in range(1, 4):
            end_copy(head, by).wait_send()
    for copy in far_copies:
        copy.wait_send()
    give_tokens.wait_send()

    @pl.when(core == 1)
    def _():
        halo_copy(0).wait_send()
        halo_copy(1).wait_send()

    @pl.when(core != kind)
    def _():
        gate_copy(0).wait_send()

    for by in range(1, 4):
        gate_copy(by).wait_send()
    for phase in range(3):
        send = (p1_send, p2_send, p3_send)[phase]
        for colour in range(3):
            every = Ring(w, pl.ds(0, CHUNKS), colour, phase, coords, core, send.at[colour], send.at[colour])
            for hop in range(2):
                every.drain(hop)


def shards(tokens, norm_gain, lru, gelu, conv_weight, conv_bias, gates, gate_bias, decay_param):
    dma = pltpu.SemaphoreType.DMA
    hbm = pl.BlockSpec(memory_space=pl.ANY)
    vmem = pl.BlockSpec(memory_space=pltpu.VMEM)
    return pl.pallas_call(
        body,
        name="branch",
        out_shape=jax.ShapeDtypeStruct((1, 512, 2048), jnp.bfloat16),
        in_specs=[hbm, vmem, hbm, hbm, vmem, vmem, hbm, vmem, vmem],
        out_specs=hbm,
        scratch_shapes=[
            pltpu.VMEM((HALO + ROWS, WIDTH), jnp.bfloat16),
            pltpu.VMEM((CHUNKS, 4, 4, 4, 64, BW), jnp.bfloat16),
            pltpu.VMEM((HEADS, BW, 2 * BW), jnp.bfloat16),
            pltpu.VMEM((HALO + ROWS, BW), jnp.float32),
            pltpu.VMEM((2, ROWS, BW), jnp.float32),
            pltpu.VMEM((2, ROWS, BW), jnp.float32),
            pltpu.VMEM((HEADS, ROWS, BW), jnp.bfloat16),
            pltpu.VMEM((HEADS, 4, 2, 8, BW), jnp.float32),
            dma((3, CHUNKS)),
            dma((3, 2, 2)),
            dma((3, 2, 2)),
            dma((3, 2, 2)),
            dma((CHUNKS, 3, 2, 2)),
            dma((3, 2, 2)),
            dma((CHUNKS, 3, 2, 2)),
            dma((3,)),
            dma((3,)),
            dma((4,)),
            dma((4,)),
            dma((HEADS, 3)),
            dma((HEADS, 3)),
            dma((2, HEADS, 2)),
            dma((HEADS, 2)),
        ],
        compiler_params=pltpu.CompilerParams(
            collective_id=0, has_side_effects=True, vmem_limit_bytes=60 * 1024 * 1024
        ),
    )(
        tokens,
        norm_gain.reshape(1, -1),
        lru,
        gelu,
        conv_weight,
        conv_bias.reshape(1, -1),
        gates,
        gate_bias,
        decay_param.reshape(1, -1),
    )


def solution(mesh):
    placed = (
        P("fsdp", "seq", None),
        P(),
        P(("fsdp", "seq"), None),
        P(("fsdp", "seq"), None),
        P(),
        P(),
        P("seq", None),
        P(),
        P(),
    )
    return jax.shard_map(
        shards, mesh=mesh, in_specs=placed, out_specs=P("fsdp", "seq", None), check_vma=False
    )
```

```python
import jax
import jax.numpy as jnp
from jax import lax
from jax.experimental import pallas as pl
from jax.experimental.pallas import tpu as pltpu
from jax.sharding import PartitionSpec as P

MESH = pl.DeviceIdType.MESH
HALO = 16
ROWS = 1024
WIDTH = 4096
HEADS = 4
BW = 256
CHUNKS = 8
X, Y, Z = 0, 1, 2
ORDERS = ((X, Y, Z), (Y, Z, X), (Z, X, Y))
PIECES = (
    (slice(0, 16), slice(0, 256)),
    (slice(16, 64), slice(0, 128)),
    (slice(16, 64), slice(128, 256)),
)
SEQUENCE = ((0, 0), (0, 1), (1, 0), (0, 2), (1, 1), (0, 3), (1, 2), (1, 3))
LRU_AT = tuple(SEQUENCE.index((0, head)) for head in range(HEADS))
GELU_AT = tuple(SEQUENCE.index((1, head)) for head in range(HEADS))
GROUPS = ((0, 2), (2, 6))
L_ROWS = 208
T_ROWS = 128
G_ROWS = 256


def piece(w, chunks, colour, phase, coords, half=None):
    order = ORDERS[colour]
    at = [chunks, None, None, None]
    for place, dim in enumerate(order):
        if place < phase:
            at[1 + dim] = pl.ds(0, 4)
            if place == 0 and half is not None:
                at[1 + dim] = pl.ds(2 * half, 2)
        else:
            at[1 + dim] = coords[dim]
    rows, cols = PIECES[colour]
    at.append(pl.ds(rows.start, rows.stop - rows.start))
    at.append(pl.ds(cols.start, cols.stop - cols.start))
    return w.at[tuple(at)]


def moved(coords, dim, by):
    new = list(coords)
    new[dim] = lax.rem(coords[dim] + (by + 4), 4)
    return new


class Ring:
    def __init__(self, w, chunks, colour, phase, coords, core, send, recv):
        self.w, self.chunks, self.colour, self.phase = w, chunks, colour, phase
        self.coords, self.core, self.send, self.recv = coords, core, send, recv
        self.dim = ORDERS[colour][phase]

    def device(self, by):
        x, y, z = moved(self.coords, self.dim, by)
        return (x * 4 + y, z * 2 + self.core)

    def block(self, by, half=None):
        chunks = self.chunks
        return piece(self.w, chunks, self.colour, self.phase, moved(self.coords, self.dim, by), half)

    def copy(self, hop, side, outgoing):
        way = 1 - 2 * side
        half = None if hop == 0 else side
        if outgoing:
            ref = self.block(-way * hop, half)
        else:
            ref = self.block(-way * (hop + 1), half)
        return pltpu.make_async_remote_copy(
            src_ref=ref,
            dst_ref=ref,
            send_sem=self.send.at[hop, side],
            recv_sem=self.recv.at[hop, side],
            device_id=self.device(way),
            device_id_type=MESH,
        )

    def start(self, hop):
        for side in range(2):
            self.copy(hop, side, True).start()

    def wait(self, hop):
        for side in range(2):
            self.copy(hop, side, False).wait_recv()

    def drain(self, hop):
        for side in range(2):
            self.copy(hop, side, True).wait_send()


def softplus_of(value):
    return jnp.maximum(value, 0.0) + jnp.log1p(jnp.exp(-jnp.abs(value)))


def one_minus_square(decay, twice):
    series = 1.0 + twice * (1.0 / 7.0)
    for divisor in (6.0, 5.0, 4.0, 3.0, 2.0):
        series = 1.0 + twice * (1.0 / divisor) * series
    return jnp.where(twice > -0.3, -twice * series, 1.0 - decay * decay)


def tile_scan(decay, driven):
    rows, cols = decay.shape
    place = lax.broadcasted_iota(jnp.int32, (rows, cols), 0)
    for step in (1, 2, 4):
        inside = (place % 8) >= step
        a_prev = jnp.where(inside, pltpu.roll(decay, step, 0), 1.0)
        b_prev = jnp.where(inside, pltpu.roll(driven, step, 0), 0.0)
        driven = decay * b_prev + driven
        decay = decay * a_prev
    group = decay.reshape(rows // 8, 8, cols)
    state = driven.reshape(rows // 8, 8, cols)
    last_a = jnp.broadcast_to(group[:, 7:8, :], group.shape)
    last_b = jnp.broadcast_to(state[:, 7:8, :], state.shape)
    run_a, run_b = last_a, last_b
    step = 1
    while step < rows // 8:
        ones = jnp.ones((step, 8, cols), jnp.float32)
        zeros = jnp.zeros((step, 8, cols), jnp.float32)
        a_prev = jnp.concatenate([ones, run_a[:-step]], axis=0)
        b_prev = jnp.concatenate([zeros, run_b[:-step]], axis=0)
        run_b = run_a * b_prev + run_b
        run_a = run_a * a_prev
        step *= 2
    ones = jnp.ones((1, 8, cols), jnp.float32)
    zeros = jnp.zeros((1, 8, cols), jnp.float32)
    before_a = jnp.concatenate([ones, run_a[:-1]], axis=0)
    before_b = jnp.concatenate([zeros, run_b[:-1]], axis=0)
    state = (state + group * before_b).reshape(rows, cols)
    group = (group * before_a).reshape(rows, cols)
    return group, state, run_a[-1], run_b[-1]


def body(
    tokens, gain, lru, gelu, conv_w, conv_b, gates, gate_b, decay_p, out,
    xn, w, stage, gate_v, rec, local, cumul, outs, ends,
    own_sem, p1_send, p1_recv, pair_recv, p2_send, p2_recv, p3_send, p3_recv,
    tok_sem, halo_sem, gate_send, gate_recv, pass_send, end_send, end_recv, out_sem, out_recv,
):
    fsdp = lax.axis_index("fsdp")
    seq = lax.axis_index("seq")
    x, y = fsdp // 4, fsdp % 4
    z, core = seq // 2, seq % 2
    other = 1 - core
    coords = [x, y, z]
    partner = (fsdp, z * 2 + other)

    def device(dim, by, on):
        nx, ny, nz = moved(coords, dim, by)
        return (nx * 4 + ny, nz * 2 + on)

    barrier = pltpu.get_barrier_semaphore()
    pl.semaphore_signal(barrier, inc=1, device_id=partner, device_id_type=MESH)
    for dim in (X, Y, Z):
        for by in (1, 2, 3):
            for on in range(2):
                pl.semaphore_signal(
                    barrier, inc=1, device_id=device(dim, by, on), device_id_type=MESH
                )

    my_part = pl.ds(pl.multiple_of(core * 32, 32), 32)
    own_copies = []
    for n, (mat, head) in enumerate(SEQUENCE):
        source = (lru, gelu)[mat]
        for mine in range(2):
            side = core if mine else other
            first = pl.multiple_of(side * (HEADS * BW) + head * BW, BW)
            dst = w.at[n, x, y, z, my_part, :] if mine else stage.at[n]
            own_copies.append(
                pltpu.make_async_copy(source.at[:, pl.ds(first, BW)], dst, own_sem.at[mine, n])
            )
    for copy in own_copies:
        copy.start()
    my_rows = pl.ds(pl.multiple_of(HALO + core * 512, 16), 512)
    my_tokens = pltpu.make_async_copy(tokens.at[0], xn.at[my_rows, :], tok_sem.at[0])
    my_tokens.start()
    for copy in own_copies:
        copy.wait()

    pl.semaphore_wait(barrier, 19)

    def first_phase(group, colour, rows):
        low, count = GROUPS[group]
        chunks = pl.ds(low, count)
        cols = pl.ds(PIECES[colour][1].start, PIECES[colour][1].stop - PIECES[colour][1].start)
        land = pl.ds(pl.multiple_of(core * 32 + rows.start, 16), rows.stop - rows.start)
        dst = w.at[chunks, x, y, z, land, cols]
        for by in (1, 3, 2):
            for on, src in (
                (core, dst),
                (other, stage.at[chunks, pl.ds(rows.start, rows.stop - rows.start), cols]),
            ):
                pltpu.make_async_remote_copy(
                    src_ref=src,
                    dst_ref=dst,
                    send_sem=p1_send,
                    recv_sem=p1_recv.at[group, colour],
                    device_id=device(ORDERS[colour][0], by, on),
                    device_id_type=MESH,
                ).start()

    def pair_phase(group):
        low, count = GROUPS[group]
        chunks = pl.ds(low, count)
        pltpu.make_async_remote_copy(
            src_ref=stage.at[chunks],
            dst_ref=w.at[chunks, x, y, z, my_part, :],
            send_sem=p1_send,
            recv_sem=pair_recv.at[group],
            device_id=partner,
            device_id_type=MESH,
        ).start()

    def first_start(group):
        @pl.when(core == 0)
        def _():
            first_phase(group, 1, slice(16, 32))
            first_phase(group, 2, slice(16, 32))
            first_phase(group, 0, slice(0, 16))

        @pl.when(core == 1)
        def _():
            first_phase(group, 1, slice(0, 32))
            first_phase(group, 2, slice(0, 32))

        pair_phase(group)

    def first_wait(group):
        low, count = GROUPS[group]
        chunks = pl.ds(low, count)
        landed = w.at[chunks, x, y, z, my_part, :]
        pltpu.make_async_copy(landed, landed, pair_recv.at[group]).wait()
        for colour in range(3):
            at = [chunks, x, y, z]
            at[1 + ORDERS[colour][0]] = pl.ds(0, 3)
            rows, cols = PIECES[colour]
            at.append(pl.ds(rows.start, rows.stop - rows.start))
            at.append(pl.ds(cols.start, cols.stop - cols.start))
            landed = w.at[tuple(at)]
            pltpu.make_async_copy(landed, landed, p1_recv.at[group, colour]).wait()

    first_start(0)
    first_start(1)

    def ring(phase, n, colour):
        send, recv = (None, (p2_send, p2_recv), (p3_send, p3_recv))[phase]
        return Ring(w, n, colour, phase, coords, core, send.at[colour], recv.at[n, colour])

    def start(phase, n, hop):
        for colour in range(3):
            ring(phase, n, colour).start(hop)

    def wait(phase, n, hop):
        for colour in range(3):
            ring(phase, n, colour).wait(hop)

    give_tokens = pltpu.make_async_remote_copy(
        src_ref=tokens.at[0],
        dst_ref=xn.at[my_rows, :],
        send_sem=tok_sem.at[1],
        recv_sem=tok_sem.at[2],
        device_id=partner,
        device_id_type=MESH,
    )
    give_tokens.start()

    def halo_copy(to_core):
        return pltpu.make_async_remote_copy(
            src_ref=tokens.at[0, pl.ds(512 - HALO, HALO), :],
            dst_ref=xn.at[pl.ds(0, HALO), :],
            send_sem=halo_sem.at[to_core],
            recv_sem=halo_sem.at[2],
            device_id=(fsdp, lax.rem(z + 1, 4) * 2 + to_core),
            device_id_type=MESH,
        )

    @pl.when(core == 1)
    def _():
        halo_copy(0).start()
        halo_copy(1).start()

    kind = z // 2
    slot = (z % 2) * 2 + core

    def gate_copy(by):
        return pltpu.make_async_remote_copy(
            src_ref=gates,
            dst_ref=gate_v.at[slot],
            send_sem=gate_send.at[by],
            recv_sem=gate_recv.at[slot, 0],
            device_id=device(Z, (0, 1, -1)[by], kind),
            device_id_type=MESH,
        )

    def gate_local():
        return pltpu.make_async_copy(gates, gate_v.at[slot], gate_recv.at[slot, 0])

    def gate_start():
        gate_copy(1).start()
        gate_copy(2).start()

        @pl.when(core == kind)
        def _():
            gate_local().start()

        @pl.when(core != kind)
        def _():
            gate_copy(0).start()

    def gate_half(j, half):
        return gate_v.at[j, pl.ds(128 * half, 128), :]

    def gate_pass(j, half):
        return pltpu.make_async_remote_copy(
            src_ref=gate_half(j, half),
            dst_ref=gate_half(j, half),
            send_sem=pass_send.at[j],
            recv_sem=gate_recv.at[j, half],
            device_id=device(Z, 1 - 2 * half, core),
            device_id_type=MESH,
        )

    def landed(ref, sem):
        pltpu.make_async_copy(ref, ref, sem).wait()

    def gate_each(act):
        for j in range(HEADS):
            away = (z + 8 - (2 * core + j // 2)) % 4
            act(j, away)

    def gate_forward(j, away):
        @pl.when(away == 0)
        def _():
            landed(gate_v.at[j], gate_recv.at[j, 0])

        @pl.when(away == 1)
        def _():
            landed(gate_v.at[j], gate_recv.at[j, 0])
            gate_pass(j, 0).start()

        @pl.when(away == 3)
        def _():
            landed(gate_v.at[j], gate_recv.at[j, 0])
            gate_pass(j, 1).start()

    def gate_end(j, away):
        @pl.when(away == 2)
        def _():
            landed(gate_half(j, 0), gate_recv.at[j, 0])
            landed(gate_half(j, 1), gate_recv.at[j, 1])

    def gate_drain(j, away):
        @pl.when(away == 1)
        def _():
            gate_pass(j, 0).wait_send()

        @pl.when(away == 3)
        def _():
            gate_pass(j, 1).wait_send()

    def norm_tile(i, _):
        rows = pl.ds(pl.multiple_of(i * 16, 16), 16)
        value = xn[rows, :].astype(jnp.float32)
        mean = jnp.mean(value * value, axis=-1, keepdims=True)
        normed = value * lax.rsqrt(mean + 1e-06) * gain[...]
        keep = jnp.where(jnp.logical_and(i == 0, z == 0), 0.0, 1.0)
        xn[rows, :] = (normed * keep).astype(jnp.bfloat16)
        return 0

    def norm(first, last):
        lax.fori_loop(first, last, norm_tile, 0)

    def p2_start(n):
        start(1, n, 0)

    def p2_pass(n):
        wait(1, n, 0)
        start(1, n, 1)

    def p3_start(n):
        wait(1, n, 1)
        start(2, n, 0)

    def p3_pass(n):
        wait(2, n, 0)
        start(2, n, 1)

    first_wait(0)
    p2_start(0)
    p2_start(1)
    first_wait(1)
    for n in (2, 3, 4):
        p2_start(n)
    my_tokens.wait()
    mine = 1 + core * 32
    norm(mine, mine + 32)
    for n in range(5):
        p2_pass(n)
    gate_start()
    give_tokens.wait_recv()
    halo_copy(0).wait_recv()
    p3_start(0)
    theirs = 1 + other * 32
    norm(theirs, theirs + 32)
    norm(0, 1)
    p3_start(1)
    gate_each(gate_forward)
    p3_pass(0)
    p3_start(2)

    def columns(head):
        return pl.ds(pl.multiple_of(core * (HEADS * BW) + head * BW, BW), BW)

    def lru_chunk(head, between):
        n = LRU_AT[head]

        def rows_of(i, _):
            rows = pl.ds(pl.multiple_of(i * L_ROWS, 16), L_ROWS)
            value = jnp.dot(
                xn[rows, :], w[n].reshape(WIDTH, BW), preferred_element_type=jnp.float32
            )
            rec[rows, :] = value.astype(jnp.bfloat16).astype(jnp.float32)
            return 0

        lax.fori_loop(0, (HALO + ROWS) // L_ROWS, rows_of, 0)
        between()
        cols = columns(head)
        taps = conv_w[:, cols]
        bias = conv_b[:, cols]
        g_bias = gate_b[:, cols]
        rate = -8.0 * softplus_of(decay_p[:, cols])
        gate_block = gates_of(head)

        def tile(i, carry):
            carry_a, carry_b = carry
            first = pl.multiple_of(i * T_ROWS + (HALO - 8), 8)
            value = rec[pl.ds(first, T_ROWS + 8), :]
            total = jnp.zeros((T_ROWS, BW), jnp.float32) + bias
            for tap in range(4):
                total = total + taps[tap : tap + 1, :] * value[8 - tap : 8 - tap + T_ROWS, :]
            conv = total.astype(jnp.bfloat16)
            gate = jnp.dot(conv, gate_block, preferred_element_type=jnp.float32)
            input_gate = jax.nn.sigmoid(gate[:, :BW] + g_bias[0:1, :])
            recur_gate = jax.nn.sigmoid(gate[:, BW:] + g_bias[1:2, :])
            log_decay = rate * recur_gate
            decay = jnp.exp(log_decay)
            driven = (
                jnp.sqrt(one_minus_square(decay, 2.0 * log_decay))
                * input_gate
                * conv.astype(jnp.float32)
            )
            within_a, within_b, tile_a, tile_b = tile_scan(decay, driven)
            rows = pl.ds(pl.multiple_of(i * T_ROWS, T_ROWS), T_ROWS)
            local[head % 2, rows, :] = within_b + within_a * carry_b[0:1, :]
            cumul[head % 2, rows, :] = within_a * carry_a[0:1, :]
            return tile_a * carry_a, tile_b + tile_a * carry_b

        begin = (jnp.ones((8, BW), jnp.float32), jnp.zeros((8, BW), jnp.float32))
        end_a, end_b = lax.fori_loop(0, ROWS // T_ROWS, tile, begin)
        ends[head, z, 0, :, :] = end_a
        ends[head, z, 1, :, :] = end_b

    def gates_of(head):
        return gate_v[head]

    def end_copy(head, by):
        return pltpu.make_async_remote_copy(
            src_ref=ends.at[head, z],
            dst_ref=ends.at[head, z],
            send_sem=end_send.at[head, by - 1],
            recv_sem=end_recv.at[head, by - 1],
            device_id=(fsdp, lax.rem(z + by, 4) * 2 + core),
            device_id_type=MESH,
        )

    def end_landed(head, by):
        source = lax.rem(z + 4 - by, 4)
        landed(ends.at[head, source], end_recv.at[head, by - 1])

    def out_copy(head, i, far):
        side = other if far else core
        src = outs.at[head, pl.ds(pl.multiple_of(side * 512 + i * G_ROWS, G_ROWS), G_ROWS), :]
        dst = out.at[0, pl.ds(i * G_ROWS, G_ROWS), columns(head)]
        if far:
            return pltpu.make_async_remote_copy(
                src_ref=src,
                dst_ref=dst,
                send_sem=out_sem.at[1, head, i],
                recv_sem=out_recv.at[head, i],
                device_id=partner,
                device_id_type=MESH,
            )
        return pltpu.make_async_copy(src, dst, out_sem.at[0, head, i])

    def gelu_chunk(head):
        n = GELU_AT[head]
        for by in range(1, 4):
            end_landed(head, by)
        begin = jnp.zeros((8, BW), jnp.float32)
        for source in range(3):
            after = ends[head, source, 0] * begin + ends[head, source, 1]
            begin = jnp.where(source < z, after, begin)
        weight = w[n].reshape(WIDTH, BW)
        for far in (True, False):
            side = other if far else core
            for i in range(2):
                first = pl.multiple_of(side * 512 + i * G_ROWS, G_ROWS)
                rows = pl.ds(first, G_ROWS)
                gelu_in = jnp.dot(
                    xn[pl.ds(pl.multiple_of(first + HALO, 16), G_ROWS), :],
                    weight,
                    preferred_element_type=jnp.float32,
                )
                state = local[head % 2, rows, :] + cumul[head % 2, rows, :] * begin[0:1, :]
                inner = gelu_in * (
                    0.7978845608028654 + (0.7978845608028654 * 0.044715) * (gelu_in * gelu_in)
                )
                part = 0.5 * gelu_in * (1.0 + jnp.tanh(inner))
                outs[head, rows, :] = (state * part).astype(jnp.bfloat16)
                out_copy(head, i, far).start()

    def before(n):
        if n + 1 < CHUNKS:
            p3_pass(n + 1)
        if n + 3 < CHUNKS:
            p3_start(n + 3)
        if n + 5 < CHUNKS:
            p2_start(n + 5)
        if n >= 1 and n + 4 < CHUNKS:
            p2_pass(n + 4)
        wait(2, n, 1)

    for n, (mat, head) in enumerate(SEQUENCE):
        before(n)
        if mat == 0:
            lru_chunk(head, (lambda: gate_each(gate_end)) if n == 0 else (lambda: None))
            for by in range(1, 4):
                end_copy(head, by).start()
        else:
            gelu_chunk(head)

    for head in range(HEADS):
        for i in range(2):
            out_copy(head, i, False).wait()
            out_copy(head, i, True).wait_send()
            first = pl.multiple_of(other * (HEADS * BW) + head * BW, BW)
            landed(out.at[0, pl.ds(i * G_ROWS, G_ROWS), pl.ds(first, BW)], out_recv.at[head, i])
        for by in range(1, 4):
            end_copy(head, by).wait_send()
    give_tokens.wait_send()

    @pl.when(core == 1)
    def _():
        halo_copy(0).wait_send()
        halo_copy(1).wait_send()

    @pl.when(core != kind)
    def _():
        gate_copy(0).wait_send()

    gate_copy(1).wait_send()
    gate_copy(2).wait_send()
    gate_each(gate_drain)
    sent = w.at[pl.ds(0, 7), x, y]
    pltpu.make_async_copy(sent, sent, p1_send).wait()
    for phase, send in ((1, p2_send), (2, p3_send)):
        for colour in range(3):
            every = Ring(w, pl.ds(0, CHUNKS), colour, phase, coords, core, send.at[colour], send.at[colour])
            for hop in range(2):
                every.drain(hop)


def shards(tokens, norm_gain, lru, gelu, conv_weight, conv_bias, gates, gate_bias, decay_param):
    dma = pltpu.SemaphoreType.DMA
    hbm = pl.BlockSpec(memory_space=pl.ANY)
    vmem = pl.BlockSpec(memory_space=pltpu.VMEM)
    return pl.pallas_call(
        body,
        name="branch",
        out_shape=jax.ShapeDtypeStruct((1, 512, 2048), jnp.bfloat16),
        in_specs=[hbm, vmem, hbm, hbm, vmem, vmem, hbm, vmem, vmem],
        out_specs=hbm,
        scratch_shapes=[
            pltpu.VMEM((HALO + ROWS, WIDTH), jnp.bfloat16),
            pltpu.VMEM((CHUNKS, 4, 4, 4, 64, BW), jnp.bfloat16),
            pltpu.VMEM((CHUNKS, 32, BW), jnp.bfloat16),
            pltpu.VMEM((HEADS, BW, 2 * BW), jnp.bfloat16),
            pltpu.VMEM((HALO + ROWS, BW), jnp.float32),
            pltpu.VMEM((2, ROWS, BW), jnp.float32),
            pltpu.VMEM((2, ROWS, BW), jnp.float32),
            pltpu.VMEM((HEADS, ROWS, BW), jnp.bfloat16),
            pltpu.VMEM((HEADS, 4, 2, 8, BW), jnp.float32),
            dma((2, CHUNKS)),
            dma,
            dma((2, 3)),
            dma((2,)),
            dma((3, 2, 2)),
            dma((CHUNKS, 3, 2, 2)),
            dma((3, 2, 2)),
            dma((CHUNKS, 3, 2, 2)),
            dma((3,)),
            dma((3,)),
            dma((3,)),
            dma((HEADS, 2)),
            dma((HEADS,)),
            dma((HEADS, 3)),
            dma((HEADS, 3)),
            dma((2, HEADS, 2)),
            dma((HEADS, 2)),
        ],
        compiler_params=pltpu.CompilerParams(
            collective_id=0, has_side_effects=True, vmem_limit_bytes=60 * 1024 * 1024
        ),
    )(
        tokens,
        norm_gain.reshape(1, -1),
        lru,
        gelu,
        conv_weight,
        conv_bias.reshape(1, -1),
        gates,
        gate_bias,
        decay_param.reshape(1, -1),
    )


def solution(mesh):
    placed = (
        P("fsdp", "seq", None),
        P(),
        P(("fsdp", "seq"), None),
        P(("fsdp", "seq"), None),
        P(),
        P(),
        P("seq", None),
        P(),
        P(),
    )
    return jax.shard_map(
        shards, mesh=mesh, in_specs=placed, out_specs=P("fsdp", "seq", None), check_vma=False
    )
```

```python
import jax
import jax.numpy as jnp
from jax import lax
from jax.experimental import pallas as pl
from jax.experimental.pallas import tpu as pltpu
from jax.sharding import PartitionSpec as P

MESH = pl.DeviceIdType.MESH
HALO = 16
ROWS = 1024
WIDTH = 4096
HEADS = 4
BW = 256
CHUNKS = 8
X, Y, Z = 0, 1, 2
USUAL = ((X, Y, Z), (Y, Z, X), (Z, X, Y))
LATE = ((X, Y, Z), (Y, Z, X), (X, Z, Y))
PIECES = (
    (slice(0, 16), slice(0, 256)),
    (slice(16, 64), slice(0, 128)),
    (slice(16, 64), slice(128, 256)),
)
SEQUENCE = ((0, 0), (0, 1), (0, 2), (1, 0), (0, 3), (1, 1), (1, 2), (1, 3))
LRU_AT = tuple(SEQUENCE.index((0, head)) for head in range(HEADS))
GELU_AT = tuple(SEQUENCE.index((1, head)) for head in range(HEADS))
GROUPS = ((0, 2, USUAL), (2, 4, USUAL), (6, 2, LATE))
PLAN = (
    ("2s", 0), ("h",), ("2s", 1), ("1p", 2), ("2f", 0), ("g0",), ("no", 0), ("no", 1), ("2f", 1), ("2s", 3),
    ("3s", 0), ("1p", 6), ("2s", 2), ("3s", 1), ("2f", 2), ("2s", 4), ("3f", 0), ("g1",), ("2s", 5), ("no", 2),
    ("no", 3), ("2f", 3), ("3f", 1), ("2s", 6), ("nt", 0), ("nt", 1), ("nt", 2), ("2f", 4), ("3s", 2),
    ("nt", 3), ("3s", 3), ("hf",), ("2f", 6), ("nh",), ("2s", 7), ("2f", 5), ("3s", 4), ("L1", 0), ("3f", 2),
    ("L2", 0), ("3f", 3), ("L1", 1), ("3s", 5), ("L2", 1), ("2f", 7), ("3f", 4), ("L1", 2), ("3s", 6),
    ("L2", 2), ("3f", 5), ("G", 3), ("3s", 7), ("L1", 4), ("3f", 6), ("L2", 4), ("G", 5), ("3f", 7), ("G", 6),
    ("G", 7),
)
ORDERS = tuple(order for _, count, order in GROUPS for _ in range(count))
NORM = 2
T_ROWS = 128


def piece(w, chunks, order, colour, phase, coords, half=None):
    at = [chunks, None, None, None]
    for place, dim in enumerate(order):
        if place < phase:
            at[1 + dim] = pl.ds(0, 4)
            if place == 0 and half is not None:
                at[1 + dim] = pl.ds(2 * half, 2)
        else:
            at[1 + dim] = coords[dim]
    rows, cols = PIECES[colour]
    at.append(pl.ds(rows.start, rows.stop - rows.start))
    at.append(pl.ds(cols.start, cols.stop - cols.start))
    return w.at[tuple(at)]


def moved(coords, dim, by):
    new = list(coords)
    new[dim] = lax.rem(coords[dim] + (by + 4), 4)
    return new


class Ring:
    def __init__(self, w, chunks, order, colour, phase, coords, core, send, recv):
        self.w, self.chunks, self.colour, self.phase = w, chunks, colour, phase
        self.coords, self.core, self.send, self.recv = coords, core, send, recv
        self.order = order
        self.dim = order[phase]

    def device(self, by):
        x, y, z = moved(self.coords, self.dim, by)
        return (x * 4 + y, z * 2 + self.core)

    def block(self, by, half=None):
        chunks = self.chunks
        return piece(self.w, chunks, self.order, self.colour, self.phase, moved(self.coords, self.dim, by), half)

    def start(self, hop, sides=(0, 1)):
        for side in sides:
            way = 1 - 2 * side
            ref = self.block(-way * hop, None if hop == 0 or self.phase == 0 else side)
            pltpu.make_async_remote_copy(
                src_ref=ref,
                dst_ref=ref,
                send_sem=self.send,
                recv_sem=self.recv,
                device_id=self.device(way),
                device_id_type=MESH,
            ).start()


def softplus_of(value):
    small = jnp.exp(-jnp.abs(value))
    ratio = small / (2.0 + small)
    square = ratio * ratio
    series = jnp.full_like(value, 1.0 / 17.0)
    for divisor in (15.0, 13.0, 11.0, 9.0, 7.0, 5.0, 3.0, 1.0):
        series = series * square + 1.0 / divisor
    return jnp.maximum(value, 0.0) + 2.0 * ratio * series


def one_minus_square(decay, twice):
    return jnp.tanh(-0.5 * twice) * (1.0 + decay * decay)


def root(value):
    return value * lax.rsqrt(jnp.maximum(value, 1e-37))


def tile_scan(decay, driven, carry_a, carry_b):
    rows, cols = decay.shape
    groups = rows // 8
    group = decay.reshape(groups, 8, cols)
    state = driven.reshape(groups, 8, cols)
    place = lax.broadcasted_iota(jnp.int32, (1, 8, cols), 1)
    for step in (1, 2, 4):
        inside = place >= step
        a_prev = jnp.where(inside, pltpu.roll(group, step, 1), 1.0)
        b_prev = jnp.where(inside, pltpu.roll(state, step, 1), 0.0)
        state = group * b_prev + state
        group = group * a_prev
    last_a = jnp.broadcast_to(group[:, 7:8, :], group.shape)
    last_b = jnp.broadcast_to(state[:, 7:8, :], state.shape)
    products, states = [], []
    for g in range(groups):
        products.append(group[g] * carry_a)
        states.append(state[g] + group[g] * carry_b)
        carry_b = last_b[g] + last_a[g] * carry_b
        carry_a = last_a[g] * carry_a
    return jnp.concatenate(products, 0), jnp.concatenate(states, 0), carry_a, carry_b


def body(
    tokens, gain, lru, gelu, conv_w, conv_b, gates, gate_b, decay_p, out,
    xn, w, stage, gate_own, gate_v, rec, local, cumul, outs, ends,
    own_sem, p1_send, p1_recv, pass_recv, pair_recv, p2_send, p2_recv, p3_send, p3_recv,
    tok_sem, halo_sem, gate_send, gate_recv, pass_send, end_send, end_recv, out_sem, out_recv,
):
    fsdp = lax.axis_index("fsdp")
    seq = lax.axis_index("seq")
    x, y = fsdp // 4, fsdp % 4
    z, core = seq // 2, seq % 2
    other = 1 - core
    coords = [x, y, z]
    partner = (fsdp, z * 2 + other)

    def device(dim, by, on):
        nx, ny, nz = moved(coords, dim, by)
        return (nx * 4 + ny, nz * 2 + on)

    barrier = pltpu.get_barrier_semaphore()
    pl.semaphore_signal(barrier, inc=1, device_id=partner, device_id_type=MESH)
    for dim in (X, Y, Z):
        for by in (1, 2, 3):
            for on in range(2):
                pl.semaphore_signal(
                    barrier, inc=1, device_id=device(dim, by, on), device_id_type=MESH
                )

    my_part = pl.ds(pl.multiple_of(core * 32, 32), 32)
    own_copies = []
    for n, (mat, head) in enumerate(SEQUENCE):
        source = (lru, gelu)[mat]
        for mine in range(2):
            side = core if mine else other
            first = pl.multiple_of(side * (HEADS * BW) + head * BW, BW)
            dst = w.at[n, x, y, z, my_part, :] if mine else stage.at[n]
            own_copies.append(
                pltpu.make_async_copy(source.at[:, pl.ds(first, BW)], dst, own_sem)
            )
    for copy in own_copies:
        copy.start()
    xn[pl.ds(0, HALO), :] = jnp.zeros((HALO, WIDTH), jnp.bfloat16)
    my_rows = pl.ds(pl.multiple_of(HALO + core * 512, 16), 512)
    my_tokens = pltpu.make_async_copy(tokens.at[0], xn.at[my_rows, :], tok_sem.at[0])
    my_tokens.start()
    stage_gate = pltpu.make_async_copy(gates, gate_own, gate_send.at[3])
    stage_gate.start()
    pltpu.make_async_copy(w.at[0, x, pl.ds(0, 2)], w.at[0, x, pl.ds(0, 2)], own_sem).wait()

    pl.semaphore_wait(barrier, 19)

    def landed(ref, sem):
        pltpu.make_async_copy(ref, ref, sem).wait()

    def first_phase(group, colour, rows):
        low, count, order = GROUPS[group]
        chunks = pl.ds(low, count)
        cols = pl.ds(PIECES[colour][1].start, PIECES[colour][1].stop - PIECES[colour][1].start)
        land = pl.ds(pl.multiple_of(core * 32 + rows.start, 16), rows.stop - rows.start)
        dst = w.at[chunks, x, y, z, land, cols]
        for by in (1, 3, 2) if group == 0 else (1, 3):
            for on, src in (
                (core, dst),
                (other, stage.at[chunks, pl.ds(rows.start, rows.stop - rows.start), cols]),
            ):
                pltpu.make_async_remote_copy(
                    src_ref=src,
                    dst_ref=dst,
                    send_sem=p1_send.at[min(group, 1)],
                    recv_sem=p1_recv.at[group],
                    device_id=device(order[colour][0], by, on),
                    device_id_type=MESH,
                ).start()

    def first_start(group):
        low, count, _ = GROUPS[group]
        chunks = pl.ds(low, count)

        @pl.when(core == 0)
        def _():
            first_phase(group, 1, slice(16, 32))
            first_phase(group, 2, slice(16, 32))
            first_phase(group, 0, slice(0, 16))

        @pl.when(core == 1)
        def _():
            first_phase(group, 1, slice(0, 32))
            first_phase(group, 2, slice(0, 32))

        pltpu.make_async_remote_copy(
            src_ref=stage.at[chunks],
            dst_ref=w.at[chunks, x, y, z, my_part, :],
            send_sem=p1_send.at[min(group, 1)],
            recv_sem=pair_recv.at[group],
            device_id=partner,
            device_id_type=MESH,
        ).start()

    def first_wait(group):
        low, count, _ = GROUPS[group]
        chips = 3 if group == 0 else 2
        landed(w.at[pl.ds(low, count), x, y, pl.ds(0, chips)], p1_recv.at[group])
        landed(w.at[pl.ds(low, count), x, y, z, my_part, :], pair_recv.at[group])

    def first_pass(group):
        low, count, order = GROUPS[group]
        half = count // 2
        for colour in range(3):
            for side in range(2):
                Ring(
                    w, pl.ds(low + half * side, half), order[colour], colour, 0, coords, core,
                    p1_send.at[2], pass_recv.at[group],
                ).start(1, (side,))

    def first_last(group):
        low, count, _ = GROUPS[group]
        landed(w.at[pl.ds(low, count), x, y, z], pass_recv.at[group])

    for group in range(3):
        first_start(group)

    def start(phase, n, hop):
        send, recv = (None, (p2_send, p2_recv), (p3_send, p3_recv))[phase]
        for colour in range(3):
            Ring(
                w, n, ORDERS[n][colour], colour, phase, coords, core, send, recv.at[n, hop]
            ).start(hop)

    def wait(phase, n, hop):
        if phase == 1:
            landed(w.at[n, x, pl.ds(0, 2 - hop)], p2_recv.at[n, hop])
        else:
            landed(w.at[n, pl.ds(0, 2 - hop)], p3_recv.at[n, hop])

    give_tokens = pltpu.make_async_remote_copy(
        src_ref=tokens.at[0],
        dst_ref=xn.at[my_rows, :],
        send_sem=tok_sem.at[1],
        recv_sem=tok_sem.at[2],
        device_id=partner,
        device_id_type=MESH,
    )

    halo_rows = xn.at[pl.ds(8, 8), :]

    def halo_out():
        return pltpu.make_async_remote_copy(
            src_ref=tokens.at[0, pl.ds(504, 8), :],
            dst_ref=halo_rows,
            send_sem=halo_sem.at[0],
            recv_sem=halo_sem.at[2],
            device_id=device(Z, 1, 1),
            device_id_type=MESH,
        )

    def halo_over():
        return pltpu.make_async_remote_copy(
            src_ref=halo_rows,
            dst_ref=halo_rows,
            send_sem=halo_sem.at[1],
            recv_sem=halo_sem.at[2],
            device_id=partner,
            device_id_type=MESH,
        )

    def halo_start():
        @pl.when(core == 1)
        def _():
            halo_out().start()

    def halo_pass():
        @pl.when(core == 1)
        def _():
            halo_out().wait_recv()
            halo_over().start()

    def halo_norm():
        @pl.when(core == 1)
        def _():
            halo_over().wait_send()

        @pl.when(core == 0)
        def _():
            halo_over().wait_recv()

        norm_rows(0, True)

    kind = z // 2
    slot = (z % 2) * 2 + core

    def gate_copy(by):
        return pltpu.make_async_remote_copy(
            src_ref=gate_own,
            dst_ref=gate_v.at[slot],
            send_sem=gate_send.at[by],
            recv_sem=gate_recv.at[slot, 0],
            device_id=device(Z, (0, 1, -1)[by], kind),
            device_id_type=MESH,
        )

    def gate_local():
        return pltpu.make_async_copy(gates, gate_v.at[slot], gate_recv.at[slot, 0])

    def gate_start():
        stage_gate.wait()
        gate_copy(1).start()
        gate_copy(2).start()

        @pl.when(core == kind)
        def _():
            gate_local().start()

        @pl.when(core != kind)
        def _():
            gate_copy(0).start()

    def gate_half(j, half):
        return gate_v.at[j, pl.ds(128 * half, 128), :]

    def gate_pass(j, half):
        return pltpu.make_async_remote_copy(
            src_ref=gate_half(j, half),
            dst_ref=gate_half(j, half),
            send_sem=pass_send.at[j],
            recv_sem=gate_recv.at[j, half],
            device_id=device(Z, 1 - 2 * half, core),
            device_id_type=MESH,
        )

    def gate_each(act):
        for j in range(HEADS):
            away = (z + 8 - (2 * core + j // 2)) % 4
            act(j, away)

    def gate_forward(j, away):
        @pl.when(away == 0)
        def _():
            landed(gate_v.at[j], gate_recv.at[j, 0])

        @pl.when(away == 1)
        def _():
            landed(gate_v.at[j], gate_recv.at[j, 0])
            gate_pass(j, 0).start()

        @pl.when(away == 3)
        def _():
            landed(gate_v.at[j], gate_recv.at[j, 0])
            gate_pass(j, 1).start()

    def gate_end(j, away):
        @pl.when(away == 2)
        def _():
            landed(gate_half(j, 0), gate_recv.at[j, 0])
            landed(gate_half(j, 1), gate_recv.at[j, 1])

    def gate_drain(j, away):
        @pl.when(away == 1)
        def _():
            gate_pass(j, 0).wait_send()

        @pl.when(away == 3)
        def _():
            gate_pass(j, 1).wait_send()

    def norm_rows(i, first):
        rows = pl.ds(pl.multiple_of(i * 16, 16), 16)
        value = xn[rows, :].astype(jnp.float32)
        mean = jnp.mean(value * value, axis=-1, keepdims=True)
        normed = value * lax.rsqrt(mean + 1e-06) * gain[...]
        if first:
            normed = normed * jnp.where(z == 0, 0.0, 1.0)
        xn[rows, :] = normed.astype(jnp.bfloat16)

    def norm(side, part):
        base = 1 + side * 32 + part * 8

        def pair(i, _):
            for k in range(NORM):
                norm_rows(base + i * NORM + k, False)
            return 0

        lax.fori_loop(0, 8 // NORM, pair, 0)

    def p2_start(n):
        start(1, n, 0)

    def p2_pass(n):
        wait(1, n, 0)
        start(1, n, 1)

    def p3_start(n):
        wait(1, n, 1)
        start(2, n, 0)

    def p3_pass(n):
        wait(2, n, 0)
        start(2, n, 1)

    def columns(head):
        return pl.ds(pl.multiple_of(core * (HEADS * BW) + head * BW, BW), BW)

    def lru_rows(head):
        n = LRU_AT[head]

        for low, high in ((0, 528), (528, HALO + ROWS)):
            value = jnp.dot(
                xn[low:high, :], w[n].reshape(WIDTH, BW), preferred_element_type=jnp.float32
            )
            rec[low:high, :] = value.astype(jnp.bfloat16).astype(jnp.float32)

    def lru_tiles(head):
        cols = columns(head)
        taps = conv_w[:, cols]
        bias = conv_b[:, cols]
        g_bias = gate_b[:, cols]
        rate = -8.0 * softplus_of(decay_p[:, cols])
        gate_block = gates_of(head)

        def tile(i, carry):
            carry_a, carry_b = carry
            first = pl.multiple_of(i * T_ROWS + (HALO - 8), 8)
            value = rec[pl.ds(first, T_ROWS + 8), :]
            total = jnp.zeros((T_ROWS, BW), jnp.float32) + bias
            for tap in range(4):
                total = total + taps[tap : tap + 1, :] * value[8 - tap : 8 - tap + T_ROWS, :]
            conv = total.astype(jnp.bfloat16)
            gate = jnp.dot(conv, gate_block, preferred_element_type=jnp.float32)
            input_gate = jax.nn.sigmoid(gate[:, :BW] + g_bias[0:1, :])
            recur_gate = jax.nn.sigmoid(gate[:, BW:] + g_bias[1:2, :])
            log_decay = rate * recur_gate
            decay = jnp.exp(log_decay)
            driven = (
                root(one_minus_square(decay, 2.0 * log_decay))
                * input_gate
                * conv.astype(jnp.float32)
            )
            rows = pl.ds(pl.multiple_of(i * T_ROWS, T_ROWS), T_ROWS)
            products, states, carry_a, carry_b = tile_scan(decay, driven, carry_a, carry_b)
            cumul[head, rows, :] = products
            local[head, rows, :] = states
            return carry_a, carry_b

        begin = (jnp.ones((8, BW), jnp.float32), jnp.zeros((8, BW), jnp.float32))
        end_a, end_b = lax.fori_loop(0, ROWS // T_ROWS, tile, begin)
        ends[head, z, 0, :, :] = end_a
        ends[head, z, 1, :, :] = end_b

    def gates_of(head):
        return gate_v[head]

    def end_copy(head, by):
        return pltpu.make_async_remote_copy(
            src_ref=ends.at[head, z],
            dst_ref=ends.at[head, z],
            send_sem=end_send,
            recv_sem=end_recv.at[head],
            device_id=(fsdp, lax.rem(z + by, 4) * 2 + core),
            device_id_type=MESH,
        )

    def ends_landed(head):
        landed(ends.at[head, pl.ds(0, 3)], end_recv.at[head])

    def out_copy(head):
        return pltpu.make_async_remote_copy(
            src_ref=outs.at[head],
            dst_ref=out.at[0, :, columns(head)],
            send_sem=out_sem,
            recv_sem=out_recv.at[head],
            device_id=partner,
            device_id_type=MESH,
        )

    def gelu_chunk(head):
        n = GELU_AT[head]
        ends_landed(head)
        begin = jnp.zeros((8, BW), jnp.float32)
        for source in range(3):
            after = ends[head, source, 0] * begin + ends[head, source, 1]
            begin = jnp.where(source < z, after, begin)
        def rows_of(side):
            first = pl.multiple_of(side * 512, 512)
            rec[pl.ds(first, 512), :] = jnp.dot(
                xn[pl.ds(pl.multiple_of(first + HALO, 16), 512), :],
                w[n].reshape(WIDTH, BW),
                preferred_element_type=jnp.float32,
            )

        start_state = begin[0:1, :]

        def part(i, side):
            rows = pl.ds(pl.multiple_of(side * 512 + i * T_ROWS, T_ROWS), T_ROWS)
            gelu_in = rec[rows, :]
            state = local[head, rows, :] + cumul[head, rows, :] * start_state
            inner = gelu_in * (
                0.7978845608028654 + (0.7978845608028654 * 0.044715) * (gelu_in * gelu_in)
            )
            gelu_out = 0.5 * gelu_in * (1.0 + jnp.tanh(inner))
            return (state * gelu_out).astype(jnp.bfloat16)

        def far_part(i, _):
            outs[head, pl.ds(pl.multiple_of(i * T_ROWS, T_ROWS), T_ROWS), :] = part(i, other)
            return 0

        def near_part(i, _):
            rows = pl.ds(pl.multiple_of(i * T_ROWS, T_ROWS), T_ROWS)
            out[0, rows, columns(head)] = part(i, core)
            return 0

        def half(i, _):
            rows_of((other + i) % 2)

            @pl.when(i == 0)
            def _():
                lax.fori_loop(0, 512 // T_ROWS, far_part, 0)
                out_copy(head).start()

            @pl.when(i == 1)
            def _():
                lax.fori_loop(0, 512 // T_ROWS, near_part, 0)

            return 0

        lax.fori_loop(0, 2, half, 0)

    def group_of(n):
        return [low + count > n for low, count, _ in GROUPS].index(True)

    waited = set()

    def once(what, act):
        if what not in waited:
            waited.add(what)
            act()

    def first_ready(group):
        if group == 0:
            first_wait(0)
        else:
            first_last(group)

    def step(kind, n=None):
        if kind == "1p":
            first_wait(group_of(n))
            first_pass(group_of(n))
        elif kind == "2s":
            once(("first", group_of(n)), lambda: first_ready(group_of(n)))
            p2_start(n)
            once("give", give_tokens.start)
        elif kind == "2f":
            p2_pass(n)
        elif kind == "3s":
            p3_start(n)
        elif kind == "3f":
            p3_pass(n)
        elif kind == "h":
            halo_start()
        elif kind == "hf":
            halo_pass()
        elif kind == "nh":
            halo_norm()
        elif kind == "g0":
            gate_start()
        elif kind == "g1":
            gate_each(gate_forward)
        elif kind == "no":
            once("mine", my_tokens.wait)
            norm(core, n)
        elif kind == "nt":
            once("theirs", give_tokens.wait_recv)
            norm(other, n)
        elif kind == "L1":
            wait(2, n, 1)
            lru_rows(SEQUENCE[n][1])
        elif kind == "L2":
            if n == 0:
                gate_each(gate_end)
            lru_tiles(SEQUENCE[n][1])
            for by in range(1, 4):
                end_copy(SEQUENCE[n][1], by).start()
        elif kind == "G":
            wait(2, n, 1)
            gelu_chunk(SEQUENCE[n][1])

    for what in PLAN:
        with jax.named_scope("s" + "_".join(str(item) for item in what)):
            step(*what)

    with jax.named_scope("outs"):
        for head in range(HEADS):
            first = pl.multiple_of(other * (HEADS * BW) + head * BW, BW)
            landed(out.at[0, :, pl.ds(first, BW)], out_recv.at[head])
    landed(outs, out_sem)
    landed(ends.at[:, pl.ds(0, 3)], end_send)
    with jax.named_scope("rest"):
        give_tokens.wait_send()

    @pl.when(core == 1)
    def _():
        halo_out().wait_send()

    @pl.when(core != kind)
    def _():
        gate_copy(0).wait_send()

    gate_copy(1).wait_send()
    gate_copy(2).wait_send()
    gate_each(gate_drain)
    landed(w.at[pl.ds(0, 7), x, y, z], p1_send.at[0])
    landed(w.at[pl.ds(0, 5), pl.ds(0, 3), y, z], p1_send.at[1])
    landed(w.at[pl.ds(0, 6), x, y, z], p1_send.at[2])
    landed(w.at[pl.ds(0, 3), pl.ds(0, 2)], p2_send)
    landed(w.at[pl.ds(0, 6)], p3_send)


def shards(tokens, norm_gain, lru, gelu, conv_weight, conv_bias, gates, gate_bias, decay_param):
    dma = pltpu.SemaphoreType.DMA
    hbm = pl.BlockSpec(memory_space=pl.ANY)
    vmem = pl.BlockSpec(memory_space=pltpu.VMEM)
    return pl.pallas_call(
        body,
        name="branch",
        out_shape=pltpu.VMEM((1, 512, 2048), jnp.bfloat16),
        in_specs=[hbm, vmem, hbm, hbm, vmem, vmem, hbm, vmem, vmem],
        out_specs=vmem,
        scratch_shapes=[
            pltpu.VMEM((HALO + ROWS, WIDTH), jnp.bfloat16),
            pltpu.VMEM((CHUNKS, 4, 4, 4, 64, BW), jnp.bfloat16),
            pltpu.VMEM((CHUNKS, 32, BW), jnp.bfloat16),
            pltpu.VMEM((BW, 2 * BW), jnp.bfloat16),
            pltpu.VMEM((HEADS, BW, 2 * BW), jnp.bfloat16),
            pltpu.VMEM((HALO + ROWS, BW), jnp.float32),
            pltpu.VMEM((HEADS, ROWS, BW), jnp.float32),
            pltpu.VMEM((HEADS, ROWS, BW), jnp.float32),
            pltpu.VMEM((HEADS, 512, BW), jnp.bfloat16),
            pltpu.VMEM((HEADS, 4, 2, 8, BW), jnp.float32),
            dma,
            dma((3,)),
            dma((3,)),
            dma((3,)),
            dma((3,)),
            dma,
            dma((CHUNKS, 2)),
            dma,
            dma((CHUNKS, 2)),
            dma((3,)),
            dma((3,)),
            dma((4,)),
            dma((HEADS, 2)),
            dma((HEADS,)),
            dma,
            dma((HEADS,)),
            dma,
            dma((HEADS,)),
        ],
        compiler_params=pltpu.CompilerParams(
            collective_id=0, has_side_effects=True, vmem_limit_bytes=56 * 1024 * 1024
        ),
    )(
        tokens,
        norm_gain.reshape(1, -1),
        lru,
        gelu,
        conv_weight,
        conv_bias.reshape(1, -1),
        gates,
        gate_bias,
        decay_param.reshape(1, -1),
    )


def solution(mesh):
    placed = (
        P("fsdp", "seq", None),
        P(),
        P(("fsdp", "seq"), None),
        P(("fsdp", "seq"), None),
        P(),
        P(),
        P("seq", None),
        P(),
        P(),
    )
    return jax.shard_map(
        shards, mesh=mesh, in_specs=placed, out_specs=P("fsdp", "seq", None), check_vma=False
    )
```

```python
import jax
import jax.numpy as jnp
from jax import lax
from jax.experimental import pallas as pl
from jax.experimental.pallas import tpu as pltpu
from jax.sharding import PartitionSpec as P

MESH = pl.DeviceIdType.MESH
HALO = 16
ROWS = 1024
WIDTH = 4096
HEADS = 4
BW = 256
CHUNKS = 8
X, Y, Z = 0, 1, 2
USUAL = ((X, Y, Z), (Y, Z, X), (Z, X, Y))
LATE = ((X, Y, Z), (Y, Z, X), (X, Z, Y))
PIECES = (
    (slice(0, 16), slice(0, 256)),
    (slice(16, 64), slice(0, 128)),
    (slice(16, 64), slice(128, 256)),
)
SEQUENCE = ((0, 0), (0, 1), (0, 2), (1, 0), (0, 3), (1, 1), (1, 2), (1, 3))
LRU_AT = tuple(SEQUENCE.index((0, head)) for head in range(HEADS))
GELU_AT = tuple(SEQUENCE.index((1, head)) for head in range(HEADS))
GROUPS = ((0, 2, USUAL), (2, 4, USUAL), (6, 2, LATE))
PLAN = (
    ("t", 1), ("g0", 0), ("1p", 2), ("2s", 0), ("no", 0), ("2s", 1), ("1p", 6), ("h",), ("2s", 3), ("2s", 2),
    ("2f", 0), ("t", 0), ("2s", 6), ("2s", 5), ("no", 1), ("2f", 1), ("2f", 3), ("2f", 2), ("hf",), ("2s", 4),
    ("3s", 0), ("t", 2), ("no", 2), ("no", 3), ("3s", 1), ("g0", 1), ("2f", 4), ("3s", 2), ("nt", 0), ("3f", 0),
    ("t", 3), ("g1", 1), ("g1", 0), ("3s", 3), ("2f", 5), ("2f", 6), ("3f", 1), ("3f", 2), ("nt", 1), ("3s", 4),
    ("nt", 2), ("2s", 7), ("nt", 3), ("nh",), ("L1", 0), ("L2", 0), ("3s", 5), ("L1", 1), ("3f", 3), ("L2", 1),
    ("3f", 4), ("L1", 2), ("2f", 7), ("3s", 6), ("L2", 2), ("3f", 5), ("G", 3), ("3s", 7), ("L1", 4), ("3f", 6),
    ("L2", 4), ("G", 5), ("3f", 7), ("G", 6), ("G", 7),
)
ORDERS = tuple(order for _, count, order in GROUPS for _ in range(count))
NORM = 8
T_ROWS = 256


def piece(w, chunks, order, colour, phase, coords, half=None):
    at = [chunks, None, None, None]
    for place, dim in enumerate(order):
        if place < phase:
            at[1 + dim] = pl.ds(0, 4)
            if place == 0 and half is not None:
                at[1 + dim] = pl.ds(2 * half, 2)
        else:
            at[1 + dim] = coords[dim]
    rows, cols = PIECES[colour]
    at.append(pl.ds(rows.start, rows.stop - rows.start))
    at.append(pl.ds(cols.start, cols.stop - cols.start))
    return w.at[tuple(at)]


def moved(coords, dim, by):
    new = list(coords)
    new[dim] = lax.rem(coords[dim] + (by + 4), 4)
    return new


class Ring:
    def __init__(self, w, chunks, order, colour, phase, coords, core, send, recv):
        self.w, self.chunks, self.colour, self.phase = w, chunks, colour, phase
        self.coords, self.core, self.send, self.recv = coords, core, send, recv
        self.order = order
        self.dim = order[phase]

    def device(self, by):
        x, y, z = moved(self.coords, self.dim, by)
        return (x * 4 + y, z * 2 + self.core)

    def block(self, by, half=None):
        chunks = self.chunks
        return piece(self.w, chunks, self.order, self.colour, self.phase, moved(self.coords, self.dim, by), half)

    def start(self, hop, sides=(0, 1)):
        for side in sides:
            way = 1 - 2 * side
            ref = self.block(-way * hop, None if hop == 0 or self.phase == 0 else side)
            pltpu.make_async_remote_copy(
                src_ref=ref,
                dst_ref=ref,
                send_sem=self.send,
                recv_sem=self.recv,
                device_id=self.device(way),
                device_id_type=MESH,
            ).start()


def softplus_of(value):
    small = jnp.exp(-jnp.abs(value))
    ratio = small / (2.0 + small)
    square = ratio * ratio
    series = jnp.full_like(value, 1.0 / 17.0)
    for divisor in (15.0, 13.0, 11.0, 9.0, 7.0, 5.0, 3.0, 1.0):
        series = series * square + 1.0 / divisor
    return jnp.maximum(value, 0.0) + 2.0 * ratio * series


def one_minus_square(decay, twice):
    return jnp.tanh(-0.5 * twice) * (1.0 + decay * decay)


def root(value):
    return value * lax.rsqrt(jnp.maximum(value, 1e-37))


def tile_scan(decay, driven, carry_a, carry_b):
    rows, cols = decay.shape
    groups = rows // 8
    group = decay.reshape(groups, 8, cols)
    state = driven.reshape(groups, 8, cols)
    place = lax.broadcasted_iota(jnp.int32, (1, 8, cols), 1)
    for step in (1, 2, 4):
        inside = place >= step
        a_prev = jnp.where(inside, pltpu.roll(group, step, 1), 1.0)
        b_prev = jnp.where(inside, pltpu.roll(state, step, 1), 0.0)
        state = group * b_prev + state
        group = group * a_prev
    last_a = jnp.broadcast_to(group[:, 7:8, :], group.shape)
    last_b = jnp.broadcast_to(state[:, 7:8, :], state.shape)
    products, states = [], []
    for g in range(groups):
        products.append(group[g] * carry_a)
        states.append(state[g] + group[g] * carry_b)
        carry_b = last_b[g] + last_a[g] * carry_b
        carry_a = last_a[g] * carry_a
    return jnp.concatenate(products, 0), jnp.concatenate(states, 0), carry_a, carry_b


def body(
    tokens, gain, lru, gelu, conv_w, conv_b, gates, gate_b, decay_p, out,
    xn, w, stage, gate_own, gate_v, rec, local, cumul, outs, ends,
    own_sem, p1_send, p1_recv, pass_recv, pair_recv, p2_send, p2_recv, p3_send, p3_recv,
    tok_sem, tok_recv, halo_sem, gate_send, gate_recv, pass_send, end_send, end_recv, out_sem, out_recv,
):
    fsdp = lax.axis_index("fsdp")
    seq = lax.axis_index("seq")
    x, y = fsdp // 4, fsdp % 4
    z, core = seq // 2, seq % 2
    other = 1 - core
    coords = [x, y, z]
    partner = (fsdp, z * 2 + other)

    def device(dim, by, on):
        nx, ny, nz = moved(coords, dim, by)
        return (nx * 4 + ny, nz * 2 + on)

    def group_at(n):
        return [low + count > n for low, count, _ in GROUPS].index(True)

    my_part = pl.ds(pl.multiple_of(core * 32, 32), 32)
    own_copies = []
    for n, (mat, head) in enumerate(SEQUENCE):
        source = (lru, gelu)[mat]
        for mine in range(2):
            side = core if mine else other
            first = pl.multiple_of(side * (HEADS * BW) + head * BW, BW)
            dst = w.at[n, x, y, z, my_part, :] if mine else stage.at[n]
            own_copies.append(
                pltpu.make_async_copy(source.at[:, pl.ds(first, BW)], dst, own_sem.at[group_at(n)])
            )
    for copy in own_copies:
        copy.start()

    xn[pl.ds(0, HALO), :] = jnp.zeros((HALO, WIDTH), jnp.bfloat16)

    barrier = pltpu.get_barrier_semaphore()
    pl.semaphore_signal(barrier, inc=1, device_id=partner, device_id_type=MESH)
    for dim in (X, Y, Z):
        for by in (1, 2, 3):
            for on in range(2):
                pl.semaphore_signal(
                    barrier, inc=1, device_id=device(dim, by, on), device_id_type=MESH
                )

    my_rows = pl.ds(pl.multiple_of(HALO + core * 512, 16), 512)
    my_tokens = pltpu.make_async_copy(tokens.at[0], xn.at[my_rows, :], tok_sem.at[0])
    my_tokens.start()
    stage_gate = pltpu.make_async_copy(gates, gate_own, gate_send.at[3])
    stage_gate.start()
    pl.semaphore_wait(barrier, 19)

    def landed(ref, sem):
        pltpu.make_async_copy(ref, ref, sem).wait()

    def first_phase(group, colour, rows):
        low, count, order = GROUPS[group]
        chunks = pl.ds(low, count)
        cols = pl.ds(PIECES[colour][1].start, PIECES[colour][1].stop - PIECES[colour][1].start)
        land = pl.ds(pl.multiple_of(core * 32 + rows.start, 16), rows.stop - rows.start)
        dst = w.at[chunks, x, y, z, land, cols]
        for by in (2, 1, 3) if group == 0 else (1, 3):
            for on, src in (
                (core, dst),
                (other, stage.at[chunks, pl.ds(rows.start, rows.stop - rows.start), cols]),
            ):
                pltpu.make_async_remote_copy(
                    src_ref=src,
                    dst_ref=dst,
                    send_sem=p1_send.at[min(group, 1)],
                    recv_sem=p1_recv.at[group],
                    device_id=device(order[colour][0], by, on),
                    device_id_type=MESH,
                ).start()

    def first_start(group):
        low, count, _ = GROUPS[group]
        chunks = pl.ds(low, count)

        @pl.when(core == 0)
        def _():
            first_phase(group, 1, slice(16, 32))
            first_phase(group, 2, slice(16, 32))
            first_phase(group, 0, slice(0, 16))

        @pl.when(core == 1)
        def _():
            first_phase(group, 1, slice(0, 32))
            first_phase(group, 2, slice(0, 32))

        pltpu.make_async_remote_copy(
            src_ref=stage.at[chunks],
            dst_ref=w.at[chunks, x, y, z, my_part, :],
            send_sem=p1_send.at[min(group, 1)],
            recv_sem=pair_recv.at[group],
            device_id=partner,
            device_id_type=MESH,
        ).start()

    def first_wait(group):
        low, count, _ = GROUPS[group]
        chips = 3 if group == 0 else 2
        landed(w.at[pl.ds(low, count), x, y, pl.ds(0, chips)], p1_recv.at[group])
        landed(w.at[pl.ds(low, count), x, y, z, my_part, :], pair_recv.at[group])

    def first_pass(group):
        low, count, order = GROUPS[group]
        half = count // 2
        for colour in range(3):
            for side in range(2):
                Ring(
                    w, pl.ds(low + half * side, half), order[colour], colour, 0, coords, core,
                    p1_send.at[2], pass_recv.at[group],
                ).start(1, (side,))

    def first_last(group):
        low, count, _ = GROUPS[group]
        landed(w.at[pl.ds(low, count), x, y, z], pass_recv.at[group])

    for group in range(3):
        pair = w.at[pl.ds(0, GROUPS[group][1]), x, y, z]
        landed(pair, own_sem.at[group])
        first_start(group)

    def start(phase, n, hop):
        send, recv = (None, (p2_send, p2_recv), (p3_send, p3_recv))[phase]
        for colour in range(3):
            Ring(
                w, n, ORDERS[n][colour], colour, phase, coords, core, send, recv.at[n, hop]
            ).start(hop)

    def wait(phase, n, hop):
        if phase == 1:
            landed(w.at[n, x, pl.ds(0, 2 - hop)], p2_recv.at[n, hop])
        else:
            landed(w.at[n, pl.ds(0, 2 - hop)], p3_recv.at[n, hop])

    def give_tokens(i):
        return pltpu.make_async_remote_copy(
            src_ref=tokens.at[0, pl.ds(i * 128, 128), :],
            dst_ref=xn.at[pl.ds(pl.multiple_of(HALO + core * 512 + i * 128, 16), 128), :],
            send_sem=tok_sem.at[1],
            recv_sem=tok_recv.at[i],
            device_id=partner,
            device_id_type=MESH,
        )

    halo_rows = xn.at[pl.ds(8, 8), :]

    def halo_out():
        return pltpu.make_async_remote_copy(
            src_ref=tokens.at[0, pl.ds(504, 8), :],
            dst_ref=halo_rows,
            send_sem=halo_sem.at[0],
            recv_sem=halo_sem.at[2],
            device_id=device(Z, 1, 1),
            device_id_type=MESH,
        )

    def halo_over():
        return pltpu.make_async_remote_copy(
            src_ref=halo_rows,
            dst_ref=halo_rows,
            send_sem=halo_sem.at[1],
            recv_sem=halo_sem.at[2],
            device_id=partner,
            device_id_type=MESH,
        )

    def halo_start():
        @pl.when(core == 1)
        def _():
            halo_out().start()

    def halo_pass():
        @pl.when(core == 1)
        def _():
            halo_out().wait_recv()
            halo_over().start()

    def halo_norm():
        @pl.when(core == 1)
        def _():
            halo_over().wait_send()

        @pl.when(core == 0)
        def _():
            halo_over().wait_recv()

        norm_rows(0, True)

    kind = z // 2
    slot = (z % 2) * 2 + core

    def gate_half(ref, half):
        return ref.at[pl.ds(128 * half, 128), :]

    def gate_copy(by, half):
        return pltpu.make_async_remote_copy(
            src_ref=gate_half(gate_own, half),
            dst_ref=gate_half(gate_v.at[slot], half),
            send_sem=gate_send.at[by],
            recv_sem=gate_recv.at[slot, half],
            device_id=device(Z, (0, 1, -1)[by], kind),
            device_id_type=MESH,
        )

    def gate_start(half):
        if half == 0:
            stage_gate.wait()
        gate_copy(1, half).start()
        gate_copy(2, half).start()

        @pl.when(core == kind)
        def _():
            pltpu.make_async_copy(
                gate_half(gates, half), gate_half(gate_v.at[slot], half), gate_recv.at[slot, half]
            ).start()

        @pl.when(core != kind)
        def _():
            gate_copy(0, half).start()

    def gate_pass(j, half):
        part = gate_half(gate_v.at[j], half)
        return pltpu.make_async_remote_copy(
            src_ref=part,
            dst_ref=part,
            send_sem=pass_send.at[j],
            recv_sem=gate_recv.at[j, half],
            device_id=device(Z, 1 - 2 * half, core),
            device_id_type=MESH,
        )

    def gate_each(act):
        for j in range(HEADS):
            away = (z + 8 - (2 * core + j // 2)) % 4
            for half in range(2):
                act(j, half, away == 1 + 2 * half)

    def gate_forward(wanted):
        def act(j, half, passed):
            if half == wanted:

                @pl.when(passed)
                def _():
                    landed(gate_half(gate_v.at[j], half), gate_recv.at[j, half])
                    gate_pass(j, half).start()

        gate_each(act)

    def gate_end(j, half, passed):
        @pl.when(jnp.logical_not(passed))
        def _():
            landed(gate_half(gate_v.at[j], half), gate_recv.at[j, half])

    def gate_drain(j, half, passed):
        @pl.when(passed)
        def _():
            gate_pass(j, half).wait_send()

    def norm_rows(i, first):
        rows = pl.ds(pl.multiple_of(i * 16, 16), 16)
        value = xn[rows, :].astype(jnp.float32)
        mean = jnp.mean(value * value, axis=-1, keepdims=True)
        normed = value * lax.rsqrt(mean + 1e-06) * gain[...]
        if first:
            normed = normed * jnp.where(z == 0, 0.0, 1.0)
        xn[rows, :] = normed.astype(jnp.bfloat16)

    def norm(side, part):
        base = 1 + side * 32 + part * 8

        def pair(i, _):
            for k in range(NORM):
                norm_rows(base + i * NORM + k, False)
            return 0

        lax.fori_loop(0, 8 // NORM, pair, 0)

    def p2_start(n):
        start(1, n, 0)

    def p2_pass(n):
        wait(1, n, 0)
        start(1, n, 1)

    def p3_start(n):
        wait(1, n, 1)
        start(2, n, 0)

    def p3_pass(n):
        wait(2, n, 0)
        start(2, n, 1)

    def columns(head):
        return pl.ds(pl.multiple_of(core * (HEADS * BW) + head * BW, BW), BW)

    def lru_rows(head):
        n = LRU_AT[head]

        for low, high in ((0, 528), (528, HALO + ROWS)):
            value = jnp.dot(
                xn[low:high, :], w[n].reshape(WIDTH, BW), preferred_element_type=jnp.float32
            )
            rec[low:high, :] = value.astype(jnp.bfloat16).astype(jnp.float32)

    def lru_tiles(head):
        cols = columns(head)
        taps = conv_w[:, cols]
        bias = conv_b[:, cols]
        g_bias = gate_b[:, cols]
        rate = -8.0 * softplus_of(decay_p[:, cols])
        gate_block = gates_of(head)

        def tile(i, carry):
            carry_a, carry_b = carry
            first = pl.multiple_of(i * T_ROWS + (HALO - 8), 8)
            value = rec[pl.ds(first, T_ROWS + 8), :]
            total = jnp.zeros((T_ROWS, BW), jnp.float32) + bias
            for tap in range(4):
                total = total + taps[tap : tap + 1, :] * value[8 - tap : 8 - tap + T_ROWS, :]
            conv = total.astype(jnp.bfloat16)
            gate = jnp.dot(conv, gate_block, preferred_element_type=jnp.float32)
            input_gate = jax.nn.sigmoid(gate[:, :BW] + g_bias[0:1, :])
            recur_gate = jax.nn.sigmoid(gate[:, BW:] + g_bias[1:2, :])
            log_decay = rate * recur_gate
            decay = jnp.exp(log_decay)
            driven = (
                root(one_minus_square(decay, 2.0 * log_decay))
                * input_gate
                * conv.astype(jnp.float32)
            )
            rows = pl.ds(pl.multiple_of(i * T_ROWS, T_ROWS), T_ROWS)
            products, states, carry_a, carry_b = tile_scan(decay, driven, carry_a, carry_b)
            cumul[head, rows, :] = products
            local[head, rows, :] = states
            return carry_a, carry_b

        begin = (jnp.ones((8, BW), jnp.float32), jnp.zeros((8, BW), jnp.float32))
        end_a, end_b = lax.fori_loop(0, ROWS // T_ROWS, tile, begin)
        ends[head, z, 0, :, :] = end_a
        ends[head, z, 1, :, :] = end_b

    def gates_of(head):
        return gate_v[head]

    def end_copy(head, by):
        return pltpu.make_async_remote_copy(
            src_ref=ends.at[head, z],
            dst_ref=ends.at[head, z],
            send_sem=end_send,
            recv_sem=end_recv.at[head],
            device_id=(fsdp, lax.rem(z + by, 4) * 2 + core),
            device_id_type=MESH,
        )

    def ends_landed(head):
        landed(ends.at[head, pl.ds(0, 3)], end_recv.at[head])

    def out_copy(head):
        return pltpu.make_async_remote_copy(
            src_ref=outs.at[head],
            dst_ref=out.at[0, :, columns(head)],
            send_sem=out_sem,
            recv_sem=out_recv.at[head],
            device_id=partner,
            device_id_type=MESH,
        )

    def gelu_chunk(head):
        n = GELU_AT[head]
        ends_landed(head)
        begin = jnp.zeros((8, BW), jnp.float32)
        for source in range(3):
            after = ends[head, source, 0] * begin + ends[head, source, 1]
            begin = jnp.where(source < z, after, begin)
        def rows_of(side):
            first = pl.multiple_of(side * 512, 512)
            rec[pl.ds(first, 512), :] = jnp.dot(
                xn[pl.ds(pl.multiple_of(first + HALO, 16), 512), :],
                w[n].reshape(WIDTH, BW),
                preferred_element_type=jnp.float32,
            )

        start_state = begin[0:1, :]

        def part(i, side):
            rows = pl.ds(pl.multiple_of(side * 512 + i * T_ROWS, T_ROWS), T_ROWS)
            gelu_in = rec[rows, :]
            state = local[head, rows, :] + cumul[head, rows, :] * start_state
            inner = gelu_in * (
                0.7978845608028654 + (0.7978845608028654 * 0.044715) * (gelu_in * gelu_in)
            )
            gelu_out = 0.5 * gelu_in * (1.0 + jnp.tanh(inner))
            return (state * gelu_out).astype(jnp.bfloat16)

        def far_part(i, _):
            outs[head, pl.ds(pl.multiple_of(i * T_ROWS, T_ROWS), T_ROWS), :] = part(i, other)
            return 0

        def near_part(i, _):
            rows = pl.ds(pl.multiple_of(i * T_ROWS, T_ROWS), T_ROWS)
            out[0, rows, columns(head)] = part(i, core)
            return 0

        def half(i, _):
            rows_of((other + i) % 2)

            @pl.when(i == 0)
            def _():
                lax.fori_loop(0, 512 // T_ROWS, far_part, 0)
                out_copy(head).start()

            @pl.when(i == 1)
            def _():
                lax.fori_loop(0, 512 // T_ROWS, near_part, 0)

            return 0

        lax.fori_loop(0, 2, half, 0)

    def group_of(n):
        return [low + count > n for low, count, _ in GROUPS].index(True)

    waited = set()

    def once(what, act):
        if what not in waited:
            waited.add(what)
            act()

    def first_ready(group):
        if group == 0:
            first_wait(0)
        else:
            first_last(group)

    def step(kind, n=None):
        if kind == "1p":
            first_wait(group_of(n))
            first_pass(group_of(n))
        elif kind == "2s":
            once(("first", group_of(n)), lambda: first_ready(group_of(n)))
            p2_start(n)
        elif kind == "2f":
            p2_pass(n)
        elif kind == "3s":
            p3_start(n)
        elif kind == "3f":
            p3_pass(n)
        elif kind == "t":
            give_tokens(n).start()
        elif kind == "h":
            halo_start()
        elif kind == "hf":
            halo_pass()
        elif kind == "nh":
            halo_norm()
        elif kind == "g0":
            gate_start(n)
        elif kind == "g1":
            gate_forward(n)
        elif kind == "no":
            once("mine", my_tokens.wait)
            norm(core, n)
        elif kind == "nt":
            give_tokens(n).wait_recv()
            norm(other, n)
        elif kind == "L1":
            wait(2, n, 1)
            lru_rows(SEQUENCE[n][1])
        elif kind == "L2":
            if n == 0:
                gate_each(gate_end)
            lru_tiles(SEQUENCE[n][1])
            for by in range(1, 4):
                end_copy(SEQUENCE[n][1], by).start()
        elif kind == "G":
            wait(2, n, 1)
            gelu_chunk(SEQUENCE[n][1])

    for what in PLAN:
        with jax.named_scope("s" + "_".join(str(item) for item in what)):
            step(*what)

    with jax.named_scope("outs"):
        for head in range(HEADS):
            first = pl.multiple_of(other * (HEADS * BW) + head * BW, BW)
            landed(out.at[0, :, pl.ds(first, BW)], out_recv.at[head])
    landed(outs, out_sem)
    landed(ends.at[:, pl.ds(0, 3)], end_send)
    with jax.named_scope("rest"):
        landed(xn.at[pl.ds(HALO, 512), :], tok_sem.at[1])

    @pl.when(core == 1)
    def _():
        halo_out().wait_send()

    @pl.when(core != kind)
    def _():
        landed(gate_own, gate_send.at[0])

    landed(gate_own, gate_send.at[1])
    landed(gate_own, gate_send.at[2])
    gate_each(gate_drain)
    landed(w.at[pl.ds(0, 7), x, y, z], p1_send.at[0])
    landed(w.at[pl.ds(0, 5), pl.ds(0, 3), y, z], p1_send.at[1])
    landed(w.at[pl.ds(0, 6), x, y, z], p1_send.at[2])
    landed(w.at[pl.ds(0, 3), pl.ds(0, 2)], p2_send)
    landed(w.at[pl.ds(0, 6)], p3_send)


def shards(tokens, norm_gain, lru, gelu, conv_weight, conv_bias, gates, gate_bias, decay_param):
    dma = pltpu.SemaphoreType.DMA
    hbm = pl.BlockSpec(memory_space=pl.ANY)
    vmem = pl.BlockSpec(memory_space=pltpu.VMEM)
    return pl.pallas_call(
        body,
        name="branch",
        out_shape=pltpu.VMEM((1, 512, 2048), jnp.bfloat16),
        in_specs=[hbm, vmem, hbm, hbm, vmem, vmem, hbm, vmem, vmem],
        out_specs=vmem,
        scratch_shapes=[
            pltpu.VMEM((HALO + ROWS, WIDTH), jnp.bfloat16),
            pltpu.VMEM((CHUNKS, 4, 4, 4, 64, BW), jnp.bfloat16),
            pltpu.VMEM((CHUNKS, 32, BW), jnp.bfloat16),
            pltpu.VMEM((BW, 2 * BW), jnp.bfloat16),
            pltpu.VMEM((HEADS, BW, 2 * BW), jnp.bfloat16),
            pltpu.VMEM((HALO + ROWS, BW), jnp.float32),
            pltpu.VMEM((HEADS, ROWS, BW), jnp.float32),
            pltpu.VMEM((HEADS, ROWS, BW), jnp.float32),
            pltpu.VMEM((HEADS, 512, BW), jnp.bfloat16),
            pltpu.VMEM((HEADS, 4, 2, 8, BW), jnp.float32),
            dma((3,)),
            dma((3,)),
            dma((3,)),
            dma((3,)),
            dma((3,)),
            dma,
            dma((CHUNKS, 2)),
            dma,
            dma((CHUNKS, 2)),
            dma((2,)),
            dma((4,)),
            dma((3,)),
            dma((4,)),
            dma((HEADS, 2)),
            dma((HEADS,)),
            dma,
            dma((HEADS,)),
            dma,
            dma((HEADS,)),
        ],
        compiler_params=pltpu.CompilerParams(
            collective_id=0, has_side_effects=True, vmem_limit_bytes=56 * 1024 * 1024
        ),
    )(
        tokens,
        norm_gain.reshape(1, -1),
        lru,
        gelu,
        conv_weight,
        conv_bias.reshape(1, -1),
        gates,
        gate_bias,
        decay_param.reshape(1, -1),
    )


def solution(mesh):
    placed = (
        P("fsdp", "seq", None),
        P(),
        P(("fsdp", "seq"), None),
        P(("fsdp", "seq"), None),
        P(),
        P(),
        P("seq", None),
        P(),
        P(),
    )
    return jax.shard_map(
        shards, mesh=mesh, in_specs=placed, out_specs=P("fsdp", "seq", None), check_vma=False
    )
```

```python
import jax
import jax.numpy as jnp
from jax import lax
from jax.experimental import pallas as pl
from jax.experimental.pallas import tpu as pltpu
from jax.sharding import PartitionSpec as P

MESH = pl.DeviceIdType.MESH
HALO = 16
ROWS = 1024
WIDTH = 4096
HEADS = 4
BW = 256
CHUNKS = 8
X, Y, Z = 0, 1, 2
USUAL = ((X, Y, Z), (Y, Z, X), (Z, X, Y))
LATE = ((X, Y, Z), (Y, Z, X), (X, Z, Y))
PIECES = (
    (slice(0, 16), slice(0, 256)),
    (slice(16, 64), slice(0, 128)),
    (slice(16, 64), slice(128, 256)),
)
SEQUENCE = ((0, 0), (0, 1), (0, 2), (1, 0), (0, 3), (1, 1), (1, 2), (1, 3))
LRU_AT = tuple(SEQUENCE.index((0, head)) for head in range(HEADS))
GELU_AT = tuple(SEQUENCE.index((1, head)) for head in range(HEADS))
GROUPS = ((0, 2, USUAL), (2, 4, USUAL), (6, 2, LATE))
PLAN = (
    ("t", 1), ("g0", 0), ("1p", 2), ("2s", 0), ("no", 0), ("2s", 1), ("1p", 6), ("h",), ("2s", 3), ("2s", 2),
    ("2f", 0), ("t", 0), ("2s", 6), ("2s", 5), ("no", 1), ("2f", 1), ("2f", 3), ("2f", 2), ("hf",), ("2s", 4),
    ("3s", 0), ("t", 2), ("no", 2), ("no", 3), ("3s", 1), ("g0", 1), ("2f", 4), ("3s", 2), ("nt", 0), ("3f", 0),
    ("t", 3), ("g1", 1), ("g1", 0), ("3s", 3), ("2f", 5), ("2f", 6), ("3f", 1), ("3f", 2), ("nt", 1), ("3s", 4),
    ("nt", 2), ("2s", 7), ("nt", 3), ("nh",), ("L1", 0), ("L2", 0), ("3s", 5), ("L1", 1), ("3f", 3), ("L2", 1),
    ("3f", 4), ("L1", 2), ("2f", 7), ("3s", 6), ("L2", 2), ("3f", 5), ("G", 3), ("3s", 7), ("L1", 4), ("3f", 6),
    ("L2", 4), ("G", 5), ("3f", 7), ("G", 6), ("G", 7),
)
ORDERS = tuple(order for _, count, order in GROUPS for _ in range(count))
NORM = 8
T_ROWS = 256


def piece(w, chunks, order, colour, phase, coords, half=None):
    at = [chunks, None, None, None]
    for place, dim in enumerate(order):
        if place < phase:
            at[1 + dim] = pl.ds(0, 4)
            if place == 0 and half is not None:
                at[1 + dim] = pl.ds(2 * half, 2)
        else:
            at[1 + dim] = coords[dim]
    rows, cols = PIECES[colour]
    at.append(pl.ds(rows.start, rows.stop - rows.start))
    at.append(pl.ds(cols.start, cols.stop - cols.start))
    return w.at[tuple(at)]


def moved(coords, dim, by):
    new = list(coords)
    new[dim] = lax.rem(coords[dim] + (by + 4), 4)
    return new


class Ring:
    def __init__(self, w, chunks, order, colour, phase, coords, core, send, recv):
        self.w, self.chunks, self.colour, self.phase = w, chunks, colour, phase
        self.coords, self.core, self.send, self.recv = coords, core, send, recv
        self.order = order
        self.dim = order[phase]

    def device(self, by):
        x, y, z = moved(self.coords, self.dim, by)
        return (x * 4 + y, z * 2 + self.core)

    def block(self, by, half=None):
        chunks = self.chunks
        return piece(self.w, chunks, self.order, self.colour, self.phase, moved(self.coords, self.dim, by), half)

    def start(self, hop, sides=(0, 1)):
        for side in sides:
            way = 1 - 2 * side
            ref = self.block(-way * hop, None if hop == 0 or self.phase == 0 else side)
            pltpu.make_async_remote_copy(
                src_ref=ref,
                dst_ref=ref,
                send_sem=self.send,
                recv_sem=self.recv,
                device_id=self.device(way),
                device_id_type=MESH,
            ).start()


def softplus_of(value):
    small = jnp.exp(-jnp.abs(value))
    ratio = small / (2.0 + small)
    square = ratio * ratio
    series = jnp.full_like(value, 1.0 / 17.0)
    for divisor in (15.0, 13.0, 11.0, 9.0, 7.0, 5.0, 3.0, 1.0):
        series = series * square + 1.0 / divisor
    return jnp.maximum(value, 0.0) + 2.0 * ratio * series


def one_minus_square(decay, twice):
    return jnp.tanh(-0.5 * twice) * (1.0 + decay * decay)


def root(value):
    return value * lax.rsqrt(jnp.maximum(value, 1e-37))


def tile_scan(decay, driven, carry_a, carry_b):
    rows, cols = decay.shape
    groups = rows // 8
    group = decay.reshape(groups, 8, cols)
    state = driven.reshape(groups, 8, cols)
    place = lax.broadcasted_iota(jnp.int32, (1, 8, cols), 1)
    for step in (1, 2, 4):
        inside = place >= step
        a_prev = jnp.where(inside, pltpu.roll(group, step, 1), 1.0)
        b_prev = jnp.where(inside, pltpu.roll(state, step, 1), 0.0)
        state = group * b_prev + state
        group = group * a_prev
    last_a = jnp.broadcast_to(group[:, 7:8, :], group.shape)
    last_b = jnp.broadcast_to(state[:, 7:8, :], state.shape)
    products, states = [], []
    for g in range(groups):
        products.append(group[g] * carry_a)
        states.append(state[g] + group[g] * carry_b)
        carry_b = last_b[g] + last_a[g] * carry_b
        carry_a = last_a[g] * carry_a
    return jnp.concatenate(products, 0), jnp.concatenate(states, 0), carry_a, carry_b


def body(
    tokens, gain_in, lru, gelu, conv_w_in, conv_b_in, gates, gate_b_in, decay_p_in, out,
    gain, conv_w, conv_b, gate_b, decay_p, small_sem, xn, w, stage, gate_own, gate_v, rec, local, cumul, outs, ends,
    own_sem, p1_send, p1_recv, pass_recv, pair_recv, p2_send, p2_recv, p3_send, p3_recv,
    tok_sem, tok_recv, halo_sem, gate_send, gate_recv, pass_send, end_send, end_recv, out_sem, out_recv,
):
    fsdp = lax.axis_index("fsdp")
    seq = lax.axis_index("seq")
    x, y = fsdp // 4, fsdp % 4
    z, core = seq // 2, seq % 2
    other = 1 - core
    coords = [x, y, z]
    partner = (fsdp, z * 2 + other)

    def device(dim, by, on):
        nx, ny, nz = moved(coords, dim, by)
        return (nx * 4 + ny, nz * 2 + on)

    def group_at(n):
        return [low + count > n for low, count, _ in GROUPS].index(True)

    xn[pl.ds(0, HALO), :] = jnp.zeros((HALO, WIDTH), jnp.bfloat16)

    barrier = pltpu.get_barrier_semaphore()
    pl.semaphore_signal(barrier, inc=1, device_id=partner, device_id_type=MESH)
    for dim in (X, Y, Z):
        for by in (1, 2, 3):
            for on in range(2):
                pl.semaphore_signal(
                    barrier, inc=1, device_id=device(dim, by, on), device_id_type=MESH
                )

    my_part = pl.ds(pl.multiple_of(core * 32, 32), 32)
    own_copies = []
    for n, (mat, head) in enumerate(SEQUENCE):
        source = (lru, gelu)[mat]
        for mine in range(2):
            side = core if mine else other
            first = pl.multiple_of(side * (HEADS * BW) + head * BW, BW)
            dst = w.at[n, x, y, z, my_part, :] if mine else stage.at[n]
            own_copies.append(
                pltpu.make_async_copy(source.at[:, pl.ds(first, BW)], dst, own_sem.at[group_at(n)])
            )
    for copy in own_copies:
        copy.start()

    small_copies = [
        pltpu.make_async_copy(src, dst, small_sem.at[i])
        for i, (src, dst) in enumerate(
            (
                (gain_in, gain),
                (conv_w_in, conv_w),
                (conv_b_in, conv_b),
                (gate_b_in, gate_b),
                (decay_p_in, decay_p),
            )
        )
    ]
    for copy in small_copies:
        copy.start()
    my_rows = pl.ds(pl.multiple_of(HALO + core * 512, 16), 512)
    my_tokens = pltpu.make_async_copy(tokens.at[0], xn.at[my_rows, :], tok_sem.at[0])
    my_tokens.start()
    stage_gate = pltpu.make_async_copy(gates, gate_own, gate_send.at[3])
    stage_gate.start()
    pl.semaphore_wait(barrier, 19)

    def landed(ref, sem):
        pltpu.make_async_copy(ref, ref, sem).wait()

    def first_phase(group, colour, rows):
        low, count, order = GROUPS[group]
        chunks = pl.ds(low, count)
        cols = pl.ds(PIECES[colour][1].start, PIECES[colour][1].stop - PIECES[colour][1].start)
        land = pl.ds(pl.multiple_of(core * 32 + rows.start, 16), rows.stop - rows.start)
        dst = w.at[chunks, x, y, z, land, cols]
        for by in (2, 1, 3) if group == 0 else (1, 3):
            for on, src in (
                (core, dst),
                (other, stage.at[chunks, pl.ds(rows.start, rows.stop - rows.start), cols]),
            ):
                pltpu.make_async_remote_copy(
                    src_ref=src,
                    dst_ref=dst,
                    send_sem=p1_send.at[min(group, 1)],
                    recv_sem=p1_recv.at[group],
                    device_id=device(order[colour][0], by, on),
                    device_id_type=MESH,
                ).start()

    def first_start(group):
        low, count, _ = GROUPS[group]
        chunks = pl.ds(low, count)

        @pl.when(core == 0)
        def _():
            first_phase(group, 1, slice(16, 32))
            first_phase(group, 2, slice(16, 32))
            first_phase(group, 0, slice(0, 16))

        @pl.when(core == 1)
        def _():
            first_phase(group, 1, slice(0, 32))
            first_phase(group, 2, slice(0, 32))

        pltpu.make_async_remote_copy(
            src_ref=stage.at[chunks],
            dst_ref=w.at[chunks, x, y, z, my_part, :],
            send_sem=p1_send.at[min(group, 1)],
            recv_sem=pair_recv.at[group],
            device_id=partner,
            device_id_type=MESH,
        ).start()

    def first_wait(group):
        low, count, _ = GROUPS[group]
        chips = 3 if group == 0 else 2
        landed(w.at[pl.ds(low, count), x, y, pl.ds(0, chips)], p1_recv.at[group])
        landed(w.at[pl.ds(low, count), x, y, z, my_part, :], pair_recv.at[group])

    def first_pass(group):
        low, count, order = GROUPS[group]
        half = count // 2
        for colour in range(3):
            for side in range(2):
                Ring(
                    w, pl.ds(low + half * side, half), order[colour], colour, 0, coords, core,
                    p1_send.at[2], pass_recv.at[group],
                ).start(1, (side,))

    def first_last(group):
        low, count, _ = GROUPS[group]
        landed(w.at[pl.ds(low, count), x, y, z], pass_recv.at[group])

    for group in range(3):
        pair = w.at[pl.ds(0, GROUPS[group][1]), x, y, z]
        landed(pair, own_sem.at[group])
        first_start(group)

    def start(phase, n, hop):
        send, recv = (None, (p2_send, p2_recv), (p3_send, p3_recv))[phase]
        for colour in range(3):
            Ring(
                w, n, ORDERS[n][colour], colour, phase, coords, core, send, recv.at[n, hop]
            ).start(hop)

    def wait(phase, n, hop):
        if phase == 1:
            landed(w.at[n, x, pl.ds(0, 2 - hop)], p2_recv.at[n, hop])
        else:
            landed(w.at[n, pl.ds(0, 2 - hop)], p3_recv.at[n, hop])

    def give_tokens(i):
        return pltpu.make_async_remote_copy(
            src_ref=tokens.at[0, pl.ds(i * 128, 128), :],
            dst_ref=xn.at[pl.ds(pl.multiple_of(HALO + core * 512 + i * 128, 16), 128), :],
            send_sem=tok_sem.at[1],
            recv_sem=tok_recv.at[i],
            device_id=partner,
            device_id_type=MESH,
        )

    halo_rows = xn.at[pl.ds(8, 8), :]

    def halo_out():
        return pltpu.make_async_remote_copy(
            src_ref=tokens.at[0, pl.ds(504, 8), :],
            dst_ref=halo_rows,
            send_sem=halo_sem.at[0],
            recv_sem=halo_sem.at[2],
            device_id=device(Z, 1, 1),
            device_id_type=MESH,
        )

    def halo_over():
        return pltpu.make_async_remote_copy(
            src_ref=halo_rows,
            dst_ref=halo_rows,
            send_sem=halo_sem.at[1],
            recv_sem=halo_sem.at[2],
            device_id=partner,
            device_id_type=MESH,
        )

    def halo_start():
        @pl.when(core == 1)
        def _():
            halo_out().start()

    def halo_pass():
        @pl.when(core == 1)
        def _():
            halo_out().wait_recv()
            halo_over().start()

    def halo_norm():
        @pl.when(core == 1)
        def _():
            halo_over().wait_send()

        @pl.when(core == 0)
        def _():
            halo_over().wait_recv()

        norm_rows(0, True)

    kind = z // 2
    slot = (z % 2) * 2 + core

    def gate_half(ref, half):
        return ref.at[pl.ds(128 * half, 128), :]

    def gate_copy(by, half):
        return pltpu.make_async_remote_copy(
            src_ref=gate_half(gate_own, half),
            dst_ref=gate_half(gate_v.at[slot], half),
            send_sem=gate_send.at[by],
            recv_sem=gate_recv.at[slot, half],
            device_id=device(Z, (0, 1, -1)[by], kind),
            device_id_type=MESH,
        )

    def gate_start(half):
        if half == 0:
            stage_gate.wait()
        gate_copy(1, half).start()
        gate_copy(2, half).start()

        @pl.when(core == kind)
        def _():
            pltpu.make_async_copy(
                gate_half(gates, half), gate_half(gate_v.at[slot], half), gate_recv.at[slot, half]
            ).start()

        @pl.when(core != kind)
        def _():
            gate_copy(0, half).start()

    def gate_pass(j, half):
        part = gate_half(gate_v.at[j], half)
        return pltpu.make_async_remote_copy(
            src_ref=part,
            dst_ref=part,
            send_sem=pass_send.at[j],
            recv_sem=gate_recv.at[j, half],
            device_id=device(Z, 1 - 2 * half, core),
            device_id_type=MESH,
        )

    def gate_each(act):
        for j in range(HEADS):
            away = (z + 8 - (2 * core + j // 2)) % 4
            for half in range(2):
                act(j, half, away == 1 + 2 * half)

    def gate_forward(wanted):
        def act(j, half, passed):
            if half == wanted:

                @pl.when(passed)
                def _():
                    landed(gate_half(gate_v.at[j], half), gate_recv.at[j, half])
                    gate_pass(j, half).start()

        gate_each(act)

    def gate_end(j, half, passed):
        @pl.when(jnp.logical_not(passed))
        def _():
            landed(gate_half(gate_v.at[j], half), gate_recv.at[j, half])

    def gate_drain(j, half, passed):
        @pl.when(passed)
        def _():
            gate_pass(j, half).wait_send()

    def norm_rows(i, first):
        rows = pl.ds(pl.multiple_of(i * 16, 16), 16)
        value = xn[rows, :].astype(jnp.float32)
        mean = jnp.mean(value * value, axis=-1, keepdims=True)
        normed = value * lax.rsqrt(mean + 1e-06) * gain[...]
        if first:
            normed = normed * jnp.where(z == 0, 0.0, 1.0)
        xn[rows, :] = normed.astype(jnp.bfloat16)

    def norm(side, part):
        base = 1 + side * 32 + part * 8

        def pair(i, _):
            for k in range(NORM):
                norm_rows(base + i * NORM + k, False)
            return 0

        lax.fori_loop(0, 8 // NORM, pair, 0)

    def p2_start(n):
        start(1, n, 0)

    def p2_pass(n):
        wait(1, n, 0)
        start(1, n, 1)

    def p3_start(n):
        wait(1, n, 1)
        start(2, n, 0)

    def p3_pass(n):
        wait(2, n, 0)
        start(2, n, 1)

    def columns(head):
        return pl.ds(pl.multiple_of(core * (HEADS * BW) + head * BW, BW), BW)

    def lru_rows(head):
        n = LRU_AT[head]

        for low, high in ((0, 528), (528, HALO + ROWS)):
            value = jnp.dot(
                xn[low:high, :], w[n].reshape(WIDTH, BW), preferred_element_type=jnp.float32
            )
            rec[low:high, :] = value.astype(jnp.bfloat16).astype(jnp.float32)

    def lru_tiles(head):
        cols = columns(head)
        taps = conv_w[:, cols]
        bias = conv_b[:, cols]
        g_bias = gate_b[:, cols]
        rate = -8.0 * softplus_of(decay_p[:, cols])
        gate_block = gates_of(head)

        def tile(i, carry):
            carry_a, carry_b = carry
            first = pl.multiple_of(i * T_ROWS + (HALO - 8), 8)
            value = rec[pl.ds(first, T_ROWS + 8), :]
            total = jnp.zeros((T_ROWS, BW), jnp.float32) + bias
            for tap in range(4):
                total = total + taps[tap : tap + 1, :] * value[8 - tap : 8 - tap + T_ROWS, :]
            conv = total.astype(jnp.bfloat16)
            gate = jnp.dot(conv, gate_block, preferred_element_type=jnp.float32)
            input_gate = jax.nn.sigmoid(gate[:, :BW] + g_bias[0:1, :])
            recur_gate = jax.nn.sigmoid(gate[:, BW:] + g_bias[1:2, :])
            log_decay = rate * recur_gate
            decay = jnp.exp(log_decay)
            driven = (
                root(one_minus_square(decay, 2.0 * log_decay))
                * input_gate
                * conv.astype(jnp.float32)
            )
            rows = pl.ds(pl.multiple_of(i * T_ROWS, T_ROWS), T_ROWS)
            products, states, carry_a, carry_b = tile_scan(decay, driven, carry_a, carry_b)
            cumul[head, rows, :] = products
            local[head, rows, :] = states
            return carry_a, carry_b

        begin = (jnp.ones((8, BW), jnp.float32), jnp.zeros((8, BW), jnp.float32))
        end_a, end_b = lax.fori_loop(0, ROWS // T_ROWS, tile, begin)
        for row, value in ((0, end_a), (4, end_b)):
            ends[head, z, row : row + 2, :] = value[0:2, :128]
            ends[head, z, row + 2 : row + 4, :] = value[0:2, 128:]

    def gates_of(head):
        return gate_v[head]

    def end_copy(head, by):
        return pltpu.make_async_remote_copy(
            src_ref=ends.at[head, z],
            dst_ref=ends.at[head, z],
            send_sem=end_send,
            recv_sem=end_recv.at[head],
            device_id=(fsdp, lax.rem(z + by, 4) * 2 + core),
            device_id_type=MESH,
        )

    def ends_landed(head):
        landed(ends.at[head, pl.ds(0, 3)], end_recv.at[head])

    def out_copy(head):
        return pltpu.make_async_remote_copy(
            src_ref=outs.at[head],
            dst_ref=out.at[0, :, columns(head)],
            send_sem=out_sem,
            recv_sem=out_recv.at[head],
            device_id=partner,
            device_id_type=MESH,
        )

    def gelu_chunk(head):
        n = GELU_AT[head]
        ends_landed(head)
        begin = jnp.zeros((1, BW), jnp.float32)
        for source in range(3):
            part_a, part_b = (
                jnp.concatenate(
                    [ends[head, source, row : row + 1, :], ends[head, source, row + 2 : row + 3, :]],
                    axis=1,
                )
                for row in (0, 4)
            )
            after = part_a * begin + part_b
            begin = jnp.where(source < z, after, begin)
        def rows_of(side):
            first = pl.multiple_of(side * 512, 512)
            rec[pl.ds(first, 512), :] = jnp.dot(
                xn[pl.ds(pl.multiple_of(first + HALO, 16), 512), :],
                w[n].reshape(WIDTH, BW),
                preferred_element_type=jnp.float32,
            )

        start_state = begin

        def part(i, side):
            rows = pl.ds(pl.multiple_of(side * 512 + i * T_ROWS, T_ROWS), T_ROWS)
            gelu_in = rec[rows, :]
            state = local[head, rows, :] + cumul[head, rows, :] * start_state
            inner = gelu_in * (
                0.7978845608028654 + (0.7978845608028654 * 0.044715) * (gelu_in * gelu_in)
            )
            gelu_out = 0.5 * gelu_in * (1.0 + jnp.tanh(inner))
            return (state * gelu_out).astype(jnp.bfloat16)

        def far_part(i, _):
            outs[head, pl.ds(pl.multiple_of(i * T_ROWS, T_ROWS), T_ROWS), :] = part(i, other)
            return 0

        def near_part(i, _):
            rows = pl.ds(pl.multiple_of(i * T_ROWS, T_ROWS), T_ROWS)
            out[0, rows, columns(head)] = part(i, core)
            return 0

        def half(i, _):
            rows_of((other + i) % 2)

            @pl.when(i == 0)
            def _():
                lax.fori_loop(0, 512 // T_ROWS, far_part, 0)
                out_copy(head).start()

            @pl.when(i == 1)
            def _():
                lax.fori_loop(0, 512 // T_ROWS, near_part, 0)

            return 0

        lax.fori_loop(0, 2, half, 0)

    def group_of(n):
        return [low + count > n for low, count, _ in GROUPS].index(True)

    waited = set()

    def once(what, act):
        if what not in waited:
            waited.add(what)
            act()

    def first_ready(group):
        if group == 0:
            first_wait(0)
        else:
            first_last(group)

    def step(kind, n=None):
        if kind == "1p":
            first_wait(group_of(n))
            first_pass(group_of(n))
        elif kind == "2s":
            once(("first", group_of(n)), lambda: first_ready(group_of(n)))
            p2_start(n)
        elif kind == "2f":
            p2_pass(n)
        elif kind == "3s":
            p3_start(n)
        elif kind == "3f":
            p3_pass(n)
        elif kind == "t":
            give_tokens(n).start()
        elif kind == "h":
            halo_start()
        elif kind == "hf":
            halo_pass()
        elif kind == "nh":
            halo_norm()
        elif kind == "g0":
            gate_start(n)
        elif kind == "g1":
            gate_forward(n)
        elif kind == "no":
            once("mine", my_tokens.wait)
            once("gain", small_copies[0].wait)
            norm(core, n)
        elif kind == "nt":
            give_tokens(n).wait_recv()
            norm(other, n)
        elif kind == "L1":
            wait(2, n, 1)
            lru_rows(SEQUENCE[n][1])
        elif kind == "L2":
            if n == 0:
                gate_each(gate_end)
                for copy in small_copies[1:]:
                    copy.wait()
            lru_tiles(SEQUENCE[n][1])
            for by in range(1, 4):
                end_copy(SEQUENCE[n][1], by).start()
        elif kind == "G":
            wait(2, n, 1)
            gelu_chunk(SEQUENCE[n][1])

    for what in PLAN:
        with jax.named_scope("s" + "_".join(str(item) for item in what)):
            step(*what)

    with jax.named_scope("outs"):
        for head in range(HEADS):
            first = pl.multiple_of(other * (HEADS * BW) + head * BW, BW)
            landed(out.at[0, :, pl.ds(first, BW)], out_recv.at[head])
    landed(outs, out_sem)
    landed(ends.at[:, pl.ds(0, 3)], end_send)
    with jax.named_scope("rest"):
        landed(xn.at[pl.ds(HALO, 512), :], tok_sem.at[1])

    @pl.when(core == 1)
    def _():
        halo_out().wait_send()

    @pl.when(core != kind)
    def _():
        landed(gate_own, gate_send.at[0])

    landed(gate_own, gate_send.at[1])
    landed(gate_own, gate_send.at[2])
    gate_each(gate_drain)
    landed(w.at[pl.ds(0, 7), x, y, z], p1_send.at[0])
    landed(w.at[pl.ds(0, 5), pl.ds(0, 3), y, z], p1_send.at[1])
    landed(w.at[pl.ds(0, 6), x, y, z], p1_send.at[2])
    landed(w.at[pl.ds(0, 3), pl.ds(0, 2)], p2_send)
    landed(w.at[pl.ds(0, 6)], p3_send)


def shards(tokens, norm_gain, lru, gelu, conv_weight, conv_bias, gates, gate_bias, decay_param):
    dma = pltpu.SemaphoreType.DMA
    hbm = pl.BlockSpec(memory_space=pl.ANY)
    vmem = pl.BlockSpec(memory_space=pltpu.VMEM)
    return pl.pallas_call(
        body,
        name="branch",
        out_shape=pltpu.VMEM((1, 512, 2048), jnp.bfloat16),
        in_specs=[hbm] * 9,
        out_specs=vmem,
        scratch_shapes=[
            pltpu.VMEM((1, WIDTH), jnp.float32),
            pltpu.VMEM((4, 2 * HEADS * BW), jnp.float32),
            pltpu.VMEM((1, 2 * HEADS * BW), jnp.float32),
            pltpu.VMEM((2, 2 * HEADS * BW), jnp.float32),
            pltpu.VMEM((1, 2 * HEADS * BW), jnp.float32),
            dma((5,)),
            pltpu.VMEM((HALO + ROWS, WIDTH), jnp.bfloat16),
            pltpu.VMEM((CHUNKS, 4, 4, 4, 64, BW), jnp.bfloat16),
            pltpu.VMEM((CHUNKS, 32, BW), jnp.bfloat16),
            pltpu.VMEM((BW, 2 * BW), jnp.bfloat16),
            pltpu.VMEM((HEADS, BW, 2 * BW), jnp.bfloat16),
            pltpu.VMEM((HALO + ROWS, BW), jnp.float32),
            pltpu.VMEM((HEADS, ROWS, BW), jnp.float32),
            pltpu.VMEM((HEADS, ROWS, BW), jnp.float32),
            pltpu.VMEM((HEADS, 512, BW), jnp.bfloat16),
            pltpu.VMEM((HEADS, 4, 8, 128), jnp.float32),
            dma((3,)),
            dma((3,)),
            dma((3,)),
            dma((3,)),
            dma((3,)),
            dma,
            dma((CHUNKS, 2)),
            dma,
            dma((CHUNKS, 2)),
            dma((2,)),
            dma((4,)),
            dma((3,)),
            dma((4,)),
            dma((HEADS, 2)),
            dma((HEADS,)),
            dma,
            dma((HEADS,)),
            dma,
            dma((HEADS,)),
        ],
        compiler_params=pltpu.CompilerParams(
            collective_id=0, has_side_effects=True, vmem_limit_bytes=56 * 1024 * 1024
        ),
    )(
        tokens,
        norm_gain.reshape(1, -1),
        lru,
        gelu,
        conv_weight,
        conv_bias.reshape(1, -1),
        gates,
        gate_bias,
        decay_param.reshape(1, -1),
    )


def solution(mesh):
    placed = (
        P("fsdp", "seq", None),
        P(),
        P(("fsdp", "seq"), None),
        P(("fsdp", "seq"), None),
        P(),
        P(),
        P("seq", None),
        P(),
        P(),
    )
    return jax.shard_map(
        shards, mesh=mesh, in_specs=placed, out_specs=P("fsdp", "seq", None), check_vma=False
    )
```

```python
import jax
import jax.numpy as jnp
from jax import lax
from jax.experimental import pallas as pl
from jax.experimental.pallas import tpu as pltpu
from jax.sharding import PartitionSpec as P

MESH = pl.DeviceIdType.MESH
HALO = 16
ROWS = 1024
WIDTH = 4096
HEADS = 4
BW = 256
CHUNKS = 8
X, Y, Z = 0, 1, 2
USUAL = ((X, Y, Z), (Y, Z, X), (Z, X, Y))
LATE = ((X, Y, Z), (Y, Z, X), (X, Z, Y))
PIECES = (
    (slice(0, 16), slice(0, 256)),
    (slice(16, 64), slice(0, 128)),
    (slice(16, 64), slice(128, 256)),
)
SEQUENCE = ((0, 0), (0, 1), (0, 2), (1, 0), (0, 3), (1, 1), (1, 2), (1, 3))
LRU_AT = tuple(SEQUENCE.index((0, head)) for head in range(HEADS))
GELU_AT = tuple(SEQUENCE.index((1, head)) for head in range(HEADS))
GROUPS = ((0, 2, USUAL), (2, 4, USUAL), (6, 2, LATE))
PLAN = (
    ("g0", 0), ("1p", 2), ("2s", 0), ("no", 0), ("t", 1), ("2s", 1), ("1p", 6), ("h",), ("2s", 3), ("2s", 2),
    ("2f", 0), ("t", 0), ("2s", 6), ("2s", 5), ("no", 1), ("2f", 1), ("2f", 3), ("2f", 2), ("hf",), ("2s", 4),
    ("3s", 0), ("t", 2), ("no", 2), ("no", 3), ("3s", 1), ("g0", 1), ("2f", 4), ("3s", 2), ("nt", 0), ("3f", 0),
    ("t", 3), ("g1", 1), ("g1", 0), ("3s", 3), ("2f", 5), ("2f", 6), ("3f", 1), ("3f", 2), ("nt", 1), ("3s", 4),
    ("nt", 2), ("2s", 7), ("nt", 3), ("nh",), ("L1", 0), ("L2", 0), ("3s", 5), ("L1", 1), ("3f", 3), ("L2", 1),
    ("3f", 4), ("L1", 2), ("2f", 7), ("3s", 6), ("L2", 2), ("3f", 5), ("G", 3), ("3s", 7), ("L1", 4), ("3f", 6),
    ("L2", 4), ("G", 5), ("3f", 7), ("G", 6), ("G", 7),
)
ORDERS = tuple(order for _, count, order in GROUPS for _ in range(count))
NORM = 8
T_ROWS = 256


def piece(w, chunks, order, colour, phase, coords, half=None):
    at = [chunks, None, None, None]
    for place, dim in enumerate(order):
        if place < phase:
            at[1 + dim] = pl.ds(0, 4)
            if place == 0 and half is not None:
                at[1 + dim] = pl.ds(2 * half, 2)
        else:
            at[1 + dim] = coords[dim]
    rows, cols = PIECES[colour]
    at.append(pl.ds(rows.start, rows.stop - rows.start))
    at.append(pl.ds(cols.start, cols.stop - cols.start))
    return w.at[tuple(at)]


def moved(coords, dim, by):
    new = list(coords)
    new[dim] = lax.rem(coords[dim] + (by + 4), 4)
    return new


class Ring:
    def __init__(self, w, chunks, order, colour, phase, coords, core, send, recv):
        self.w, self.chunks, self.colour, self.phase = w, chunks, colour, phase
        self.coords, self.core, self.send, self.recv = coords, core, send, recv
        self.order = order
        self.dim = order[phase]

    def device(self, by):
        x, y, z = moved(self.coords, self.dim, by)
        return (x * 4 + y, z * 2 + self.core)

    def block(self, by, half=None):
        chunks = self.chunks
        return piece(self.w, chunks, self.order, self.colour, self.phase, moved(self.coords, self.dim, by), half)

    def start(self, hop, sides=(0, 1)):
        for side in sides:
            way = 1 - 2 * side
            ref = self.block(-way * hop, None if hop == 0 or self.phase == 0 else side)
            pltpu.make_async_remote_copy(
                src_ref=ref,
                dst_ref=ref,
                send_sem=self.send,
                recv_sem=self.recv,
                device_id=self.device(way),
                device_id_type=MESH,
            ).start()


def softplus_of(value):
    small = jnp.exp(-jnp.abs(value))
    ratio = small / (2.0 + small)
    square = ratio * ratio
    series = jnp.full_like(value, 1.0 / 17.0)
    for divisor in (15.0, 13.0, 11.0, 9.0, 7.0, 5.0, 3.0, 1.0):
        series = series * square + 1.0 / divisor
    return jnp.maximum(value, 0.0) + 2.0 * ratio * series


def one_minus_square(decay, twice):
    return jnp.tanh(-0.5 * twice) * (1.0 + decay * decay)


def root(value):
    return value * lax.rsqrt(jnp.maximum(value, 1e-37))


def tile_scan(decay, driven, carry_a, carry_b):
    rows, cols = decay.shape
    groups = rows // 8
    group = decay.reshape(groups, 8, cols)
    state = driven.reshape(groups, 8, cols)
    place = lax.broadcasted_iota(jnp.int32, (1, 8, cols), 1)
    for step in (1, 2, 4):
        inside = place >= step
        a_prev = jnp.where(inside, pltpu.roll(group, step, 1), 1.0)
        b_prev = jnp.where(inside, pltpu.roll(state, step, 1), 0.0)
        state = group * b_prev + state
        group = group * a_prev
    last_a = jnp.broadcast_to(group[:, 7:8, :], group.shape)
    last_b = jnp.broadcast_to(state[:, 7:8, :], state.shape)
    products, states = [], []
    for g in range(groups):
        products.append(group[g] * carry_a)
        states.append(state[g] + group[g] * carry_b)
        carry_b = last_b[g] + last_a[g] * carry_b
        carry_a = last_a[g] * carry_a
    return jnp.concatenate(products, 0), jnp.concatenate(states, 0), carry_a, carry_b


def body(
    tokens, gain_in, lru, gelu, conv_w_in, conv_b_in, gates, gate_b_in, decay_p_in, out,
    gain, conv_w, conv_b, gate_b, decay_p, small_sem, xn, w, stage, gate_own, gate_v, rec, local, cumul, outs, ends,
    own_sem, p1_send, p1_recv, pass_recv, pair_recv, p2_send, p2_recv, p3_send, p3_recv,
    tok_sem, tok_recv, halo_sem, gate_send, gate_recv, pass_send, end_send, end_recv, out_sem, out_recv,
):
    fsdp = lax.axis_index("fsdp")
    seq = lax.axis_index("seq")
    x, y = fsdp // 4, fsdp % 4
    z, core = seq // 2, seq % 2
    other = 1 - core
    coords = [x, y, z]
    partner = (fsdp, z * 2 + other)

    def device(dim, by, on):
        nx, ny, nz = moved(coords, dim, by)
        return (nx * 4 + ny, nz * 2 + on)

    def group_at(n):
        return [low + count > n for low, count, _ in GROUPS].index(True)

    xn[pl.ds(0, HALO), :] = jnp.zeros((HALO, WIDTH), jnp.bfloat16)

    barrier = pltpu.get_barrier_semaphore()
    pl.semaphore_signal(barrier, inc=1, device_id=partner, device_id_type=MESH)
    for dim in (X, Y, Z):
        for by in (1, 2, 3):
            for on in range(2):
                pl.semaphore_signal(
                    barrier, inc=1, device_id=device(dim, by, on), device_id_type=MESH
                )

    my_part = pl.ds(pl.multiple_of(core * 32, 32), 32)
    own_copies = []
    for n, (mat, head) in enumerate(SEQUENCE):
        source = (lru, gelu)[mat]
        for mine in range(2):
            side = core if mine else other
            first = pl.multiple_of(side * (HEADS * BW) + head * BW, BW)
            dst = w.at[n, x, y, z, my_part, :] if mine else stage.at[n]
            own_copies.append(
                pltpu.make_async_copy(source.at[:, pl.ds(first, BW)], dst, own_sem.at[group_at(n)])
            )
    for copy in own_copies:
        copy.start()

    small_copies = [
        pltpu.make_async_copy(src, dst, small_sem.at[i])
        for i, (src, dst) in enumerate(
            (
                (gain_in, gain),
                (conv_w_in, conv_w),
                (conv_b_in, conv_b),
                (gate_b_in, gate_b),
                (decay_p_in, decay_p),
            )
        )
    ]
    for copy in small_copies:
        copy.start()
    my_rows = pl.ds(pl.multiple_of(HALO + core * 512, 16), 512)
    my_tokens = pltpu.make_async_copy(tokens.at[0], xn.at[my_rows, :], tok_sem.at[0])
    my_tokens.start()
    stage_gate = pltpu.make_async_copy(gates, gate_own, gate_send.at[3])
    stage_gate.start()
    pl.semaphore_wait(barrier, 19)

    def landed(ref, sem):
        pltpu.make_async_copy(ref, ref, sem).wait()

    def first_phase(group, colour, rows):
        low, count, order = GROUPS[group]
        chunks = pl.ds(low, count)
        cols = pl.ds(PIECES[colour][1].start, PIECES[colour][1].stop - PIECES[colour][1].start)
        land = pl.ds(pl.multiple_of(core * 32 + rows.start, 16), rows.stop - rows.start)
        dst = w.at[chunks, x, y, z, land, cols]
        for by in (2, 1, 3) if group == 0 else (1, 3):
            for on, src in (
                (core, dst),
                (other, stage.at[chunks, pl.ds(rows.start, rows.stop - rows.start), cols]),
            ):
                pltpu.make_async_remote_copy(
                    src_ref=src,
                    dst_ref=dst,
                    send_sem=p1_send.at[min(group, 1)],
                    recv_sem=p1_recv.at[group],
                    device_id=device(order[colour][0], by, on),
                    device_id_type=MESH,
                ).start()

    def first_start(group):
        low, count, _ = GROUPS[group]
        chunks = pl.ds(low, count)

        @pl.when(core == 0)
        def _():
            first_phase(group, 1, slice(16, 32))
            first_phase(group, 2, slice(16, 32))
            first_phase(group, 0, slice(0, 16))

        @pl.when(core == 1)
        def _():
            first_phase(group, 1, slice(0, 32))
            first_phase(group, 2, slice(0, 32))

        pltpu.make_async_remote_copy(
            src_ref=stage.at[chunks],
            dst_ref=w.at[chunks, x, y, z, my_part, :],
            send_sem=p1_send.at[min(group, 1)],
            recv_sem=pair_recv.at[group],
            device_id=partner,
            device_id_type=MESH,
        ).start()

    def first_wait(group):
        low, count, _ = GROUPS[group]
        chips = 3 if group == 0 else 2
        landed(w.at[pl.ds(low, count), x, y, pl.ds(0, chips)], p1_recv.at[group])
        landed(w.at[pl.ds(low, count), x, y, z, my_part, :], pair_recv.at[group])

    def first_pass(group):
        low, count, order = GROUPS[group]
        half = count // 2
        for colour in range(3):
            for side in range(2):
                Ring(
                    w, pl.ds(low + half * side, half), order[colour], colour, 0, coords, core,
                    p1_send.at[2], pass_recv.at[group],
                ).start(1, (side,))

    def first_last(group):
        low, count, _ = GROUPS[group]
        landed(w.at[pl.ds(low, count), x, y, z], pass_recv.at[group])

    for group in range(3):
        pair = w.at[pl.ds(0, GROUPS[group][1]), x, y, z]
        landed(pair, own_sem.at[group])
        first_start(group)

    def start(phase, n, hop):
        send, recv = (None, (p2_send, p2_recv), (p3_send, p3_recv))[phase]
        for colour in range(3):
            Ring(
                w, n, ORDERS[n][colour], colour, phase, coords, core, send, recv.at[n, hop]
            ).start(hop)

    def wait(phase, n, hop):
        if phase == 1:
            landed(w.at[n, x, pl.ds(0, 2 - hop)], p2_recv.at[n, hop])
        else:
            landed(w.at[n, pl.ds(0, 2 - hop)], p3_recv.at[n, hop])

    def give_tokens(i):
        return pltpu.make_async_remote_copy(
            src_ref=tokens.at[0, pl.ds(i * 128, 128), :],
            dst_ref=xn.at[pl.ds(pl.multiple_of(HALO + core * 512 + i * 128, 16), 128), :],
            send_sem=tok_sem.at[1],
            recv_sem=tok_recv.at[i],
            device_id=partner,
            device_id_type=MESH,
        )

    halo_rows = xn.at[pl.ds(8, 8), :]

    def halo_out():
        return pltpu.make_async_remote_copy(
            src_ref=tokens.at[0, pl.ds(504, 8), :],
            dst_ref=halo_rows,
            send_sem=halo_sem.at[0],
            recv_sem=halo_sem.at[2],
            device_id=device(Z, 1, 1),
            device_id_type=MESH,
        )

    def halo_over():
        return pltpu.make_async_remote_copy(
            src_ref=halo_rows,
            dst_ref=halo_rows,
            send_sem=halo_sem.at[1],
            recv_sem=halo_sem.at[2],
            device_id=partner,
            device_id_type=MESH,
        )

    def halo_start():
        @pl.when(core == 1)
        def _():
            halo_out().start()

    def halo_pass():
        @pl.when(core == 1)
        def _():
            halo_out().wait_recv()
            halo_over().start()

    def halo_norm():
        @pl.when(core == 1)
        def _():
            halo_over().wait_send()

        @pl.when(core == 0)
        def _():
            halo_over().wait_recv()

        norm_rows(0, True)

    kind = z // 2
    slot = (z % 2) * 2 + core

    def gate_half(ref, half):
        return ref.at[pl.ds(128 * half, 128), :]

    def gate_copy(by, half):
        return pltpu.make_async_remote_copy(
            src_ref=gate_half(gate_own, half),
            dst_ref=gate_half(gate_v.at[slot], half),
            send_sem=gate_send.at[by],
            recv_sem=gate_recv.at[slot, half],
            device_id=device(Z, (0, 1, -1)[by], kind),
            device_id_type=MESH,
        )

    def gate_start(half):
        if half == 0:
            stage_gate.wait()
        gate_copy(1, half).start()
        gate_copy(2, half).start()

        @pl.when(core == kind)
        def _():
            pltpu.make_async_copy(
                gate_half(gates, half), gate_half(gate_v.at[slot], half), gate_recv.at[slot, half]
            ).start()

        @pl.when(core != kind)
        def _():
            gate_copy(0, half).start()

    def gate_pass(j, half):
        part = gate_half(gate_v.at[j], half)
        return pltpu.make_async_remote_copy(
            src_ref=part,
            dst_ref=part,
            send_sem=pass_send.at[j],
            recv_sem=gate_recv.at[j, half],
            device_id=device(Z, 1 - 2 * half, core),
            device_id_type=MESH,
        )

    def gate_each(act):
        for j in range(HEADS):
            away = (z + 8 - (2 * core + j // 2)) % 4
            for half in range(2):
                act(j, half, away == 1 + 2 * half)

    def gate_forward(wanted):
        def act(j, half, passed):
            if half == wanted:

                @pl.when(passed)
                def _():
                    landed(gate_half(gate_v.at[j], half), gate_recv.at[j, half])
                    gate_pass(j, half).start()

        gate_each(act)

    def gate_end(j, half, passed):
        @pl.when(jnp.logical_not(passed))
        def _():
            landed(gate_half(gate_v.at[j], half), gate_recv.at[j, half])

    def gate_drain(j, half, passed):
        @pl.when(passed)
        def _():
            gate_pass(j, half).wait_send()

    def norm_rows(i, first):
        rows = pl.ds(pl.multiple_of(i * 16, 16), 16)
        value = xn[rows, :].astype(jnp.float32)
        mean = jnp.mean(value * value, axis=-1, keepdims=True)
        normed = value * lax.rsqrt(mean + 1e-06) * gain[...]
        if first:
            normed = normed * jnp.where(z == 0, 0.0, 1.0)
        xn[rows, :] = normed.astype(jnp.bfloat16)

    def norm(side, part):
        base = 1 + side * 32 + part * 8

        def pair(i, _):
            for k in range(NORM):
                norm_rows(base + i * NORM + k, False)
            return 0

        lax.fori_loop(0, 8 // NORM, pair, 0)

    def p2_start(n):
        start(1, n, 0)

    def p2_pass(n):
        wait(1, n, 0)
        start(1, n, 1)

    def p3_start(n):
        wait(1, n, 1)
        start(2, n, 0)

    def p3_pass(n):
        wait(2, n, 0)
        start(2, n, 1)

    def columns(head):
        return pl.ds(pl.multiple_of(core * (HEADS * BW) + head * BW, BW), BW)

    def lru_rows(head):
        n = LRU_AT[head]

        for low, high in ((0, 528), (528, HALO + ROWS)):
            value = jnp.dot(
                xn[low:high, :], w[n].reshape(WIDTH, BW), preferred_element_type=jnp.float32
            )
            rec[low:high, :] = value.astype(jnp.bfloat16).astype(jnp.float32)

    def lru_tiles(head):
        cols = columns(head)
        taps = conv_w[:, cols]
        bias = conv_b[:, cols]
        g_bias = gate_b[:, cols]
        rate = -8.0 * softplus_of(decay_p[:, cols])
        gate_block = gates_of(head)

        def tile(i, carry):
            carry_a, carry_b = carry
            first = pl.multiple_of(i * T_ROWS + (HALO - 8), 8)
            value = rec[pl.ds(first, T_ROWS + 8), :]
            total = jnp.zeros((T_ROWS, BW), jnp.float32) + bias
            for tap in range(4):
                total = total + taps[tap : tap + 1, :] * value[8 - tap : 8 - tap + T_ROWS, :]
            conv = total.astype(jnp.bfloat16)
            gate = jnp.dot(conv, gate_block, preferred_element_type=jnp.float32)
            input_gate = jax.nn.sigmoid(gate[:, :BW] + g_bias[0:1, :])
            recur_gate = jax.nn.sigmoid(gate[:, BW:] + g_bias[1:2, :])
            log_decay = rate * recur_gate
            decay = jnp.exp(log_decay)
            driven = (
                root(one_minus_square(decay, 2.0 * log_decay))
                * input_gate
                * conv.astype(jnp.float32)
            )
            rows = pl.ds(pl.multiple_of(i * T_ROWS, T_ROWS), T_ROWS)
            products, states, carry_a, carry_b = tile_scan(decay, driven, carry_a, carry_b)
            cumul[head, rows, :] = products
            local[head, rows, :] = states
            return carry_a, carry_b

        begin = (jnp.ones((8, BW), jnp.float32), jnp.zeros((8, BW), jnp.float32))
        end_a, end_b = lax.fori_loop(0, ROWS // T_ROWS, tile, begin)
        for row, value in ((0, end_a), (4, end_b)):
            ends[head, z, row : row + 2, :] = value[0:2, :128]
            ends[head, z, row + 2 : row + 4, :] = value[0:2, 128:]

    def gates_of(head):
        return gate_v[head]

    def end_copy(head, by):
        return pltpu.make_async_remote_copy(
            src_ref=ends.at[head, z],
            dst_ref=ends.at[head, z],
            send_sem=end_send,
            recv_sem=end_recv.at[head],
            device_id=(fsdp, lax.rem(z + by, 4) * 2 + core),
            device_id_type=MESH,
        )

    def ends_landed(head):
        landed(ends.at[head, pl.ds(0, 3)], end_recv.at[head])

    def out_copy(head):
        return pltpu.make_async_remote_copy(
            src_ref=outs.at[head],
            dst_ref=out.at[0, :, columns(head)],
            send_sem=out_sem,
            recv_sem=out_recv.at[head],
            device_id=partner,
            device_id_type=MESH,
        )

    def gelu_chunk(head):
        n = GELU_AT[head]
        ends_landed(head)
        begin = jnp.zeros((1, BW), jnp.float32)
        for source in range(3):
            part_a, part_b = (
                jnp.concatenate(
                    [ends[head, source, row : row + 1, :], ends[head, source, row + 2 : row + 3, :]],
                    axis=1,
                )
                for row in (0, 4)
            )
            after = part_a * begin + part_b
            begin = jnp.where(source < z, after, begin)
        def rows_of(side):
            first = pl.multiple_of(side * 512, 512)
            rec[pl.ds(first, 512), :] = jnp.dot(
                xn[pl.ds(pl.multiple_of(first + HALO, 16), 512), :],
                w[n].reshape(WIDTH, BW),
                preferred_element_type=jnp.float32,
            )

        start_state = begin

        def part(i, side):
            rows = pl.ds(pl.multiple_of(side * 512 + i * T_ROWS, T_ROWS), T_ROWS)
            gelu_in = rec[rows, :]
            state = local[head, rows, :] + cumul[head, rows, :] * start_state
            inner = gelu_in * (
                0.7978845608028654 + (0.7978845608028654 * 0.044715) * (gelu_in * gelu_in)
            )
            gelu_out = 0.5 * gelu_in * (1.0 + jnp.tanh(inner))
            return (state * gelu_out).astype(jnp.bfloat16)

        def far_part(i, _):
            outs[head, pl.ds(pl.multiple_of(i * T_ROWS, T_ROWS), T_ROWS), :] = part(i, other)
            return 0

        def near_part(i, _):
            rows = pl.ds(pl.multiple_of(i * T_ROWS, T_ROWS), T_ROWS)
            out[0, rows, columns(head)] = part(i, core)
            return 0

        def half(i, _):
            rows_of((other + i) % 2)

            @pl.when(i == 0)
            def _():
                lax.fori_loop(0, 512 // T_ROWS, far_part, 0)
                out_copy(head).start()

            @pl.when(i == 1)
            def _():
                lax.fori_loop(0, 512 // T_ROWS, near_part, 0)

            return 0

        lax.fori_loop(0, 2, half, 0)

    def group_of(n):
        return [low + count > n for low, count, _ in GROUPS].index(True)

    waited = set()

    def once(what, act):
        if what not in waited:
            waited.add(what)
            act()

    def first_ready(group):
        if group == 0:
            first_wait(0)
        else:
            first_last(group)

    def step(kind, n=None):
        if kind == "1p":
            first_wait(group_of(n))
            first_pass(group_of(n))
        elif kind == "2s":
            once(("first", group_of(n)), lambda: first_ready(group_of(n)))
            p2_start(n)
        elif kind == "2f":
            p2_pass(n)
        elif kind == "3s":
            p3_start(n)
        elif kind == "3f":
            p3_pass(n)
        elif kind == "t":
            give_tokens(n).start()
        elif kind == "h":
            halo_start()
        elif kind == "hf":
            halo_pass()
        elif kind == "nh":
            halo_norm()
        elif kind == "g0":
            gate_start(n)
        elif kind == "g1":
            gate_forward(n)
        elif kind == "no":
            once("mine", my_tokens.wait)
            once("gain", small_copies[0].wait)
            norm(core, n)
        elif kind == "nt":
            give_tokens(n).wait_recv()
            norm(other, n)
        elif kind == "L1":
            wait(2, n, 1)
            lru_rows(SEQUENCE[n][1])
        elif kind == "L2":
            if n == 0:
                gate_each(gate_end)
                for copy in small_copies[1:]:
                    copy.wait()
            lru_tiles(SEQUENCE[n][1])
            for by in range(1, 4):
                end_copy(SEQUENCE[n][1], by).start()
        elif kind == "G":
            wait(2, n, 1)
            gelu_chunk(SEQUENCE[n][1])

    for what in PLAN:
        with jax.named_scope("s" + "_".join(str(item) for item in what)):
            step(*what)

    with jax.named_scope("outs"):
        for head in range(HEADS):
            first = pl.multiple_of(other * (HEADS * BW) + head * BW, BW)
            landed(out.at[0, :, pl.ds(first, BW)], out_recv.at[head])
    landed(outs, out_sem)
    landed(ends.at[:, pl.ds(0, 3)], end_send)
    with jax.named_scope("rest"):
        landed(xn.at[pl.ds(HALO, 512), :], tok_sem.at[1])

    @pl.when(core == 1)
    def _():
        halo_out().wait_send()

    @pl.when(core != kind)
    def _():
        landed(gate_own, gate_send.at[0])

    landed(gate_own, gate_send.at[1])
    landed(gate_own, gate_send.at[2])
    gate_each(gate_drain)
    landed(w.at[pl.ds(0, 7), x, y, z], p1_send.at[0])
    landed(w.at[pl.ds(0, 5), pl.ds(0, 3), y, z], p1_send.at[1])
    landed(w.at[pl.ds(0, 6), x, y, z], p1_send.at[2])
    landed(w.at[pl.ds(0, 3), pl.ds(0, 2)], p2_send)
    landed(w.at[pl.ds(0, 6)], p3_send)


def shards(tokens, norm_gain, lru, gelu, conv_weight, conv_bias, gates, gate_bias, decay_param):
    dma = pltpu.SemaphoreType.DMA
    hbm = pl.BlockSpec(memory_space=pl.ANY)
    vmem = pl.BlockSpec(memory_space=pltpu.VMEM)
    return pl.pallas_call(
        body,
        name="branch",
        out_shape=pltpu.VMEM((1, 512, 2048), jnp.bfloat16),
        in_specs=[hbm] * 9,
        out_specs=vmem,
        scratch_shapes=[
            pltpu.VMEM((1, WIDTH), jnp.float32),
            pltpu.VMEM((4, 2 * HEADS * BW), jnp.float32),
            pltpu.VMEM((1, 2 * HEADS * BW), jnp.float32),
            pltpu.VMEM((2, 2 * HEADS * BW), jnp.float32),
            pltpu.VMEM((1, 2 * HEADS * BW), jnp.float32),
            dma((5,)),
            pltpu.VMEM((HALO + ROWS, WIDTH), jnp.bfloat16),
            pltpu.VMEM((CHUNKS, 4, 4, 4, 64, BW), jnp.bfloat16),
            pltpu.VMEM((CHUNKS, 32, BW), jnp.bfloat16),
            pltpu.VMEM((BW, 2 * BW), jnp.bfloat16),
            pltpu.VMEM((HEADS, BW, 2 * BW), jnp.bfloat16),
            pltpu.VMEM((HALO + ROWS, BW), jnp.float32),
            pltpu.VMEM((HEADS, ROWS, BW), jnp.float32),
            pltpu.VMEM((HEADS, ROWS, BW), jnp.float32),
            pltpu.VMEM((HEADS, 512, BW), jnp.bfloat16),
            pltpu.VMEM((HEADS, 4, 8, 128), jnp.float32),
            dma((3,)),
            dma((3,)),
            dma((3,)),
            dma((3,)),
            dma((3,)),
            dma,
            dma((CHUNKS, 2)),
            dma,
            dma((CHUNKS, 2)),
            dma((2,)),
            dma((4,)),
            dma((3,)),
            dma((4,)),
            dma((HEADS, 2)),
            dma((HEADS,)),
            dma,
            dma((HEADS,)),
            dma,
            dma((HEADS,)),
        ],
        compiler_params=pltpu.CompilerParams(
            collective_id=0, has_side_effects=True, vmem_limit_bytes=56 * 1024 * 1024
        ),
    )(
        tokens,
        norm_gain.reshape(1, -1),
        lru,
        gelu,
        conv_weight,
        conv_bias.reshape(1, -1),
        gates,
        gate_bias,
        decay_param.reshape(1, -1),
    )


def solution(mesh):
    placed = (
        P("fsdp", "seq", None),
        P(),
        P(("fsdp", "seq"), None),
        P(("fsdp", "seq"), None),
        P(),
        P(),
        P("seq", None),
        P(),
        P(),
    )
    return jax.shard_map(
        shards, mesh=mesh, in_specs=placed, out_specs=P("fsdp", "seq", None), check_vma=False
    )
```
